128 devices in a mesh: rows: 8 (over x, core), cols: 16 (over z, y).
Axes of the slice: x: 4, y: 4, z: 4, core: 2. Of those that a mesh axis runs over, the one named last changes fastest.
Arguments:
- samples: bfloat16 [4096, 65536], P('rows', 'cols'), may hold values from -0.0234375 to 0.0234375
- labels: int32 [4096], P('rows'), may hold values 0 or 1
- weights: float32 [65536], P('cols'), may hold values from -7 to 7, as said below
- hist_s: float32 [16, 65536], P(None, 'cols'), may hold values from -60 to 60
- hist_y: float32 [16, 65536], P(None, 'cols'), may hold values from -480 to 480, as said below
- counter: int32 [1], replicated, may hold values from 0 to 4095
Outputs:
- new_weights: float32 [65536], P('cols')
- gradient: float32 [65536], P('cols')
The draws below stay inside these ranges and needn't reach their ends.
Inputs may be any that keep to these rules, and one draw needn't show every extreme that they name: weights share a common direction with the rows of hist_s. Each entry of hist_y[j] is a positive multiple of the same entry of hist_s[j], so s_j . y_j > 0.
All inputs are finite; a program needn't handle non-finite values. No bound on the sum of `labels` on one device may be relied on, other than what follows from the above.
Results may differ from the reference program's by a relative error of at most 0.0013.
Values sent between devices are 32-bit elements; how exact they have to be, the bound alone decides.
No kernel may reach another device: no remote copies, remote signals or barrier semaphores. Data moves between devices by JAX's collectives and lax.ppermute only.
A program may use at most 64 MiB of HBM per device.

```python
import math
import jax
import jax.numpy as jnp
from jax import lax

FEAT = 65536
HIST = 16
SAMPLES = 4096


def common_base(key):
    return jax.random.truncated_normal(jax.random.fold_in(key, 101), -4.0, 4.0, (FEAT,), jnp.float32)


def draw_weights(key, part):
    base = common_base(key)
    noise = jax.random.truncated_normal(jax.random.fold_in(key, 103), -4.0, 4.0, (FEAT,), jnp.float32)
    return base + 0.5 * noise


def draw_hist_s(key, part):
    base = common_base(key)
    mixing = jax.random.uniform(jax.random.fold_in(key, 107), (HIST, 1), jnp.float32, -1.0, 1.0)
    noise = jax.random.truncated_normal(jax.random.fold_in(key, 109), -4.0, 4.0, (HIST, FEAT), jnp.float32)
    field = mixing * base[None, :] + 0.5 * noise
    return field


def draw_hist_y(key, part):
    field = draw_hist_s(key, part)
    factor = jnp.exp(jax.random.uniform(jax.random.fold_in(key, 127), (HIST, FEAT), jnp.float32, math.log(0.5), math.log(4.0)))
    return factor * field


def touch_ends(array, key, least, top_value):
    longest = array.shape.index(max(array.shape))
    spots = []
    for shift in (0, 1):
        where = [jax.random.randint(jax.random.fold_in(key, axis), (), 0, length) for axis, length in enumerate(array.shape)]
        where[longest] = (where[longest] + shift) % array.shape[longest]
        spots.append(tuple(where))
    return array.at[spots[0]].set(least).at[spots[1]].set(top_value)


def shard_levels(key, dims, shards, low, top_value):
    factor_of, own = 1.0, jax.random.fold_in(key, 6)
    for position, parts in shards:
        steps = jnp.exp(jax.random.uniform(jax.random.fold_in(own, position), (parts,), jnp.float32, low / len(shards), top_value / len(shards)))
        factor_of = factor_of * jnp.repeat(steps, dims[position] // parts).reshape([-1 if axis == position else 1 for axis in range(len(dims))])
    return factor_of


def scatter_about(rng, extent, scale, limit, cuts=(), held_as=jnp.bfloat16):
    factor_of = shard_levels(rng, extent, cuts, -0.22, 0.18) if cuts else 1.0
    drawn = jax.random.normal(rng, extent, jnp.float32) * scale * factor_of
    return jnp.minimum(jnp.maximum(drawn, -limit), limit).astype(held_as)


def setup_inputs(seed: int = 0) -> dict:
    key_list = jax.random.split(jax.random.key(seed), 7)
    samples = scatter_about(key_list[0], (SAMPLES, FEAT), FEAT ** -0.5, 0.0234375, ((0, 8), (1, 16)))
    labels = touch_ends((jax.random.randint(key_list[1], (SAMPLES,), 0, 2) < 1).astype(jnp.int32), jax.random.fold_in(key_list[1], 1), 0, 1)
    weights = draw_weights(jax.random.fold_in(key_list[6], 71), 0)
    hist_s = draw_hist_s(jax.random.fold_in(key_list[6], 71), 0)
    hist_y = draw_hist_y(jax.random.fold_in(key_list[6], 71), 0)
    counter = jax.random.randint(key_list[5], (1,), 0, 4096).astype(jnp.int32)
    return {"samples": samples, "labels": labels, "weights": weights, "hist_s": hist_s, "hist_y": hist_y, "counter": counter}


penalty = 4.0
step_length = 0.5


def pick(table, slot):
    return lax.dynamic_index_in_dim(table, slot, 0, keepdims=False)


def reference(samples, labels, weights, hist_s, hist_y, counter):
    margin = jnp.dot(samples, weights.astype(jnp.bfloat16), preferred_element_type=jnp.float32)
    resid = (jax.nn.sigmoid(margin) - labels.astype(jnp.float32)).astype(jnp.bfloat16)
    total = jnp.dot(resid, samples, preferred_element_type=jnp.float32)
    gradient = weights + penalty * total
    newest = (counter[0] % HIST).astype(jnp.int32)
    curv = jnp.sum(hist_s * hist_y, axis=1)
    rho = 1.0 / curv
    y_new = pick(hist_y, newest)
    gamma = pick(curv, newest) / jnp.sum(y_new * y_new)
    query = gradient
    coefs = []
    slots = []
    for step in range(HIST):
        slot = ((newest - step) % HIST).astype(jnp.int32)
        slots.append(slot)
        coef = pick(rho, slot) * jnp.sum(pick(hist_s, slot) * query)
        coefs.append(coef)
        query = query - coef * pick(hist_y, slot)
    result = gamma * query
    for step in reversed(range(HIST)):
        slot = slots[step]
        beta = pick(rho, slot) * jnp.sum(pick(hist_y, slot) * result)
        result = result + (coefs[step] - beta) * pick(hist_s, slot)
    return weights - step_length * result, gradient
```

```python
import jax
import jax.numpy as jnp
from jax import lax
from jax.experimental import pallas as pl
from jax.experimental.pallas import tpu as pltpu
from jax.sharding import PartitionSpec as P

HIST = 16
ROWS = "rows"
COLS = "cols"
CHUNKS = 8

penalty = 4.0
step_length = 0.5
f32 = jnp.float32
bf16 = jnp.bfloat16
highest = lax.Precision.HIGHEST


def iota(shape, axis):
    return lax.broadcasted_iota(jnp.int32, shape, axis)


def dot_t(left, right):
    return lax.dot_general(left, right, (((1,), (1,)), ((), ())), preferred_element_type=f32)


def first_kernel(s_hbm, w_hbm, hs_hbm, hy_hbm, samp, hist, wrow, part, sems):
    feats = samp.shape[1]
    width = feats // CHUNKS
    copies = [
        pltpu.make_async_copy(hs_hbm, hist.at[pl.ds(0, HIST), :], sems.at[0]),
        pltpu.make_async_copy(hy_hbm, hist.at[pl.ds(HIST, HIST), :], sems.at[1]),
        pltpu.make_async_copy(w_hbm, wrow, sems.at[2]),
    ]
    for c in range(CHUNKS):
        cols = pl.ds(c * width, width)
        copies.append(pltpu.make_async_copy(s_hbm.at[:, cols], samp.at[:, cols], sems.at[3 + c]))
    for copy in copies:
        copy.start()
    for copy in copies[:3]:
        copy.wait()
    h = hist[...]
    high = h.astype(bf16)
    low = (h - high.astype(f32)).astype(bf16)
    y_high = high[HIST:]
    y_low = low[HIST:]
    right = jnp.concatenate([y_high] * 8 + [y_low] * 8, axis=0)
    left = jnp.concatenate([high, low], axis=0)
    both = dot_t(left, right)
    gram = (both[:32, 128:] + both[32:, :128]) + both[:32, :128]
    mask = iota((32, 128), 1) // HIST == iota((32, 128), 0) % 8
    gram = jnp.where(mask, gram, 0.0)
    packed = [jnp.sum(gram[8 * a : 8 * a + 8], axis=0, keepdims=True) for a in range(4)]

    acc = jnp.zeros((16, samp.shape[0]), f32)
    for c in range(CHUNKS):
        copies[3 + c].wait()
        cols = slice(c * width, (c + 1) * width)
        w16 = jnp.broadcast_to(wrow[:, cols].astype(bf16), (16, width))
        acc = acc + dot_t(w16, samp[:, cols])
    rows = [acc[0:1, 128 * i : 128 * i + 128] for i in range(4)]
    mine = jnp.concatenate(rows + packed, axis=0)
    part[...] = jnp.broadcast_to(mine[None], part.shape)


def second_kernel(parts, labels, samp, hist, wrow, total, cross, gram):
    summed = jnp.sum(parts[...], axis=0)
    gram[...] = summed
    margin = jnp.concatenate([summed[i : i + 1] for i in range(4)], axis=1)
    resid = (jax.nn.sigmoid(margin) - labels[...].astype(f32)).astype(bf16)
    resid16 = jnp.broadcast_to(resid, (16, resid.shape[1]))
    feats = samp.shape[1]
    width = 512
    acc = jnp.zeros((2 * HIST, 128), f32)
    for c in range(feats // width):
        cols = slice(c * width, (c + 1) * width)
        t = jnp.dot(resid16, samp[:, cols], preferred_element_type=f32)[0:1]
        total[:, cols] = t
        lead = wrow[:, cols] * 0.125 + penalty * t
        prod = hist[:, cols] * lead
        for k in range(width // 128):
            acc = acc + prod[:, 128 * k : 128 * k + 128]
    square = jnp.concatenate([acc, jnp.zeros((96, 128), f32)], axis=0)
    line = jnp.sum(square.T, axis=0, keepdims=True)
    cross[...] = jnp.broadcast_to(line[None], cross.shape)


def solve_kernel(counter, gram, out):
    newest = lax.rem(counter[0], HIST)
    row = iota((HIST, 128), 0)
    lane = iota((HIST, 128), 1)
    low_lane = lane < HIST

    def unpacked(a):
        kept = jnp.where(iota((8, 128), 1) // HIST == iota((8, 128), 0), gram[4 + a : 5 + a, :], 0.0)
        for shift in (16, 32, 64):
            kept = kept + pltpu.roll(kept, shift, 1)
        return kept

    sy = jnp.where(low_lane, jnp.concatenate([unpacked(0), unpacked(1)], axis=0), 0.0)
    yy = jnp.where(low_lane, jnp.concatenate([unpacked(2), unpacked(3)], axis=0), 0.0)
    diag = row == lane
    is_new = jnp.logical_and(diag, row == newest)
    pick = lambda m: jnp.sum(jnp.sum(jnp.where(is_new, m, 0.0), axis=0, keepdims=True), axis=1, keepdims=True)
    gamma = pick(sy) / pick(yy)
    rank = lax.rem(newest - row + HIST, HIST)
    curv = jnp.sum(jnp.where(diag, sy, 0.0), axis=1, keepdims=True)
    rho = 1.0 / curv
    inv = diag.astype(f32)
    for step in range(HIST):
        here = row == lax.rem(newest - step + HIST, HIST)
        there = lane == lax.rem(newest - step + HIST, HIST)
        line = jnp.sum(jnp.where(here, inv * rho, 0.0), axis=0, keepdims=True)
        column = jnp.sum(jnp.where(there, sy, 0.0), axis=1, keepdims=True)
        later = inv - column * line
        inv = jnp.where(here, jnp.broadcast_to(line, inv.shape), jnp.where(rank > step, later, inv))
    pad = jnp.zeros((128 - HIST, 128), f32)
    inv_t = jnp.concatenate([inv, pad], axis=0).T[:HIST]
    middle = gamma * yy + jnp.where(diag, sy, 0.0)
    inner = jnp.dot(middle, jnp.concatenate([inv, pad], axis=0), precision=highest, preferred_element_type=f32)
    corner = jnp.dot(inv_t, jnp.concatenate([inner, pad], axis=0), precision=highest, preferred_element_type=f32)
    out[0:HIST, :] = corner - gamma * pltpu.roll(inv_t, HIST, 1)
    out[HIST : 2 * HIST, :] = -gamma * inv
    out[2 * HIST :, :] = jnp.broadcast_to(gamma, (8, 128))


def last_kernel(crosses, solve, total, wrow, hist, new_weights, gradient):
    line = jnp.sum(crosses[...], axis=0)
    coefs = jnp.sum(solve[0 : 2 * HIST, :] * line, axis=1, keepdims=True)
    gamma = solve[2 * HIST : 2 * HIST + 1, 0:1]
    weights = wrow[...]
    grad = weights + penalty * total[...]
    gradient[...] = grad
    mixed = jnp.sum(hist[...] * coefs, axis=0, keepdims=True)
    new_weights[...] = weights - step_length * (gamma * grad + mixed)


def swapped(array, mask):
    count = lax.axis_size(ROWS)
    return array + lax.ppermute(array, ROWS, [(i, i ^ mask) for i in range(count)])


SMALL = pltpu.CompilerParams(vmem_limit_bytes=16 * 1024 * 1024)
VM = pl.BlockSpec(memory_space=pltpu.VMEM)
HB = pl.BlockSpec(memory_space=pltpu.HBM)


def body(samples, labels, weights, hist_s, hist_y, counter):
    count, feats = samples.shape
    samp, hist, wrow, part = pl.pallas_call(
        first_kernel,
        in_specs=[HB, HB, HB, HB],
        out_specs=[VM, VM, VM, VM],
        out_shape=[
            pltpu.VMEM((count, feats), bf16),
            pltpu.VMEM((2 * HIST, feats), f32),
            pltpu.VMEM((1, feats), f32),
            pltpu.VMEM((16, 8, 128), f32),
        ],
        scratch_shapes=[pltpu.SemaphoreType.DMA((3 + CHUNKS,))],
        compiler_params=SMALL,
        name="first",
    )(samples, weights.reshape(1, feats), hist_s, hist_y)
    parts = lax.all_to_all(part, COLS, split_axis=0, concat_axis=0, tiled=True)
    total, cross, gram = pl.pallas_call(
        second_kernel,
        in_specs=[VM] * 5,
        out_specs=[VM] * 3,
        out_shape=[
            pltpu.VMEM((1, feats), f32),
            pltpu.VMEM((128, 1, 128), f32),
            pltpu.VMEM((8, 128), f32),
        ],
        compiler_params=SMALL,
        name="second",
    )(parts, labels.reshape(1, count), samp, hist, wrow)
    crosses = lax.all_to_all(cross, (ROWS, COLS), split_axis=0, concat_axis=0, tiled=True)
    for mask in (7, 3, 1):
        total = swapped(total, mask)
    solve = pl.pallas_call(
        solve_kernel,
        in_specs=[pl.BlockSpec(memory_space=pltpu.SMEM), VM],
        out_specs=VM,
        out_shape=pltpu.VMEM((40, 128), f32),
        compiler_params=SMALL,
        name="solve",
    )(counter, gram)
    new_weights, gradient = pl.pallas_call(
        last_kernel,
        in_specs=[VM] * 5,
        out_specs=[VM] * 2,
        out_shape=[jax.ShapeDtypeStruct((1, feats), f32)] * 2,
        compiler_params=SMALL,
        name="last",
    )(crosses, solve, total, wrow, hist)
    return new_weights.reshape(feats), gradient.reshape(feats)


def solution(mesh):
    return jax.shard_map(
        body,
        mesh=mesh,
        in_specs=(P(ROWS, COLS), P(ROWS), P(COLS), P(None, COLS), P(None, COLS), P()),
        out_specs=(P(COLS), P(COLS)),
        check_vma=False,
    )
```

```python
import jax
import jax.numpy as jnp
from jax import lax
from jax.experimental import pallas as pl
from jax.experimental.pallas import tpu as pltpu
from jax.sharding import PartitionSpec as P

HIST = 16
ROWS = "rows"
COLS = "cols"
CHUNKS = 8

penalty = 4.0
step_length = 0.5
f32 = jnp.float32
bf16 = jnp.bfloat16
highest = lax.Precision.HIGHEST


def iota(shape, axis):
    return lax.broadcasted_iota(jnp.int32, shape, axis)


def dot_t(left, right):
    return lax.dot_general(left, right, (((1,), (1,)), ((), ())), preferred_element_type=f32)


def first_kernel(s_hbm, w_hbm, hs_hbm, hy_hbm, samp, hist, wrow, part, sems):
    feats = samp.shape[1]
    width = feats // CHUNKS
    copies = [
        pltpu.make_async_copy(hs_hbm, hist.at[pl.ds(0, HIST), :], sems.at[0]),
        pltpu.make_async_copy(hy_hbm, hist.at[pl.ds(HIST, HIST), :], sems.at[1]),
        pltpu.make_async_copy(w_hbm, wrow, sems.at[2]),
    ]
    for c in range(CHUNKS):
        cols = pl.ds(c * width, width)
        copies.append(pltpu.make_async_copy(s_hbm.at[:, cols], samp.at[:, cols], sems.at[3 + c]))
    for copy in copies:
        copy.start()
    for copy in copies[:3]:
        copy.wait()
    h = hist[...]
    high = h.astype(bf16)
    low = (h - high.astype(f32)).astype(bf16)
    y_high = high[HIST:]
    y_low = low[HIST:]
    right = jnp.concatenate([y_high] * 8 + [y_low] * 8, axis=0)
    left = jnp.concatenate([high, low], axis=0)
    both = dot_t(left, right)
    gram = (both[:32, 128:] + both[32:, :128]) + both[:32, :128]
    mask = iota((32, 128), 1) // HIST == iota((32, 128), 0) % 8
    gram = jnp.where(mask, gram, 0.0)
    packed = [jnp.sum(gram[8 * a : 8 * a + 8], axis=0, keepdims=True) for a in range(4)]

    acc = jnp.zeros((16, samp.shape[0]), f32)
    for c in range(CHUNKS):
        copies[3 + c].wait()
        cols = slice(c * width, (c + 1) * width)
        w16 = jnp.broadcast_to(wrow[:, cols].astype(bf16), (16, width))
        acc = acc + dot_t(w16, samp[:, cols])
    rows = [acc[0:1, 128 * i : 128 * i + 128] for i in range(4)]
    mine = jnp.concatenate(rows + packed, axis=0)
    part[...] = jnp.broadcast_to(mine[None], part.shape)


def second_kernel(parts, labels, samp, hist, wrow, total, cross, gram):
    summed = jnp.sum(parts[...], axis=0)
    gram[...] = summed
    margin = jnp.concatenate([summed[i : i + 1] for i in range(4)], axis=1)
    resid = (jax.nn.sigmoid(margin) - labels[...].astype(f32)).astype(bf16)
    resid16 = jnp.broadcast_to(resid, (16, resid.shape[1]))
    feats = samp.shape[1]
    width = 512
    acc = jnp.zeros((2 * HIST, 128), f32)
    for c in range(feats // width):
        cols = slice(c * width, (c + 1) * width)
        t = jnp.dot(resid16, samp[:, cols], preferred_element_type=f32)[0:1]
        total[:, cols] = t
        lead = wrow[:, cols] * 0.125 + penalty * t
        prod = hist[:, cols] * lead
        for k in range(width // 128):
            acc = acc + prod[:, 128 * k : 128 * k + 128]
    square = jnp.concatenate([acc, jnp.zeros((96, 128), f32)], axis=0)
    line = jnp.sum(square.T, axis=0, keepdims=True)
    cross[...] = jnp.broadcast_to(line[None], cross.shape)


def solve_kernel(counter, gram, out):
    newest = lax.rem(counter[0], HIST)
    row = iota((HIST, 128), 0)
    lane = iota((HIST, 128), 1)
    low_lane = lane < HIST

    def unpacked(a):
        kept = jnp.where(iota((8, 128), 1) // HIST == iota((8, 128), 0), gram[4 + a : 5 + a, :], 0.0)
        for shift in (16, 32, 64):
            kept = kept + pltpu.roll(kept, shift, 1)
        return kept

    sy = jnp.where(low_lane, jnp.concatenate([unpacked(0), unpacked(1)], axis=0), 0.0)
    yy = jnp.where(low_lane, jnp.concatenate([unpacked(2), unpacked(3)], axis=0), 0.0)
    diag = row == lane
    is_new = jnp.logical_and(diag, row == newest)
    pick = lambda m: jnp.sum(jnp.sum(jnp.where(is_new, m, 0.0), axis=0, keepdims=True), axis=1, keepdims=True)
    gamma = pick(sy) / pick(yy)
    rank = lax.rem(newest - row + HIST, HIST)
    curv = jnp.sum(jnp.where(diag, sy, 0.0), axis=1, keepdims=True)
    rho = 1.0 / curv
    inv = diag.astype(f32)
    for step in range(HIST):
        here = row == lax.rem(newest - step + HIST, HIST)
        there = lane == lax.rem(newest - step + HIST, HIST)
        line = jnp.sum(jnp.where(here, inv * rho, 0.0), axis=0, keepdims=True)
        column = jnp.sum(jnp.where(there, sy, 0.0), axis=1, keepdims=True)
        later = inv - column * line
        inv = jnp.where(here, jnp.broadcast_to(line, inv.shape), jnp.where(rank > step, later, inv))
    pad = jnp.zeros((128 - HIST, 128), f32)
    inv_t = jnp.concatenate([inv, pad], axis=0).T[:HIST]
    middle = gamma * yy + jnp.where(diag, sy, 0.0)
    inner = jnp.dot(middle, jnp.concatenate([inv, pad], axis=0), precision=highest, preferred_element_type=f32)
    corner = jnp.dot(inv_t, jnp.concatenate([inner, pad], axis=0), precision=highest, preferred_element_type=f32)
    out[0:HIST, :] = corner - gamma * pltpu.roll(inv_t, HIST, 1)
    out[HIST : 2 * HIST, :] = -gamma * inv
    out[2 * HIST :, :] = jnp.broadcast_to(gamma, (8, 128))


def last_kernel(crosses, solve, total, wrow, hist, new_weights, gradient):
    line = jnp.sum(crosses[...], axis=0)
    coefs = jnp.sum(solve[0 : 2 * HIST, :] * line, axis=1, keepdims=True)
    gamma = solve[2 * HIST : 2 * HIST + 1, 0:1]
    weights = wrow[...]
    grad = weights + penalty * total[...]
    gradient[...] = grad
    mixed = jnp.sum(hist[...] * coefs, axis=0, keepdims=True)
    new_weights[...] = weights - step_length * (gamma * grad + mixed)


def swapped(array, mask):
    count = lax.axis_size(ROWS)
    return array + lax.ppermute(array, ROWS, [(i, i ^ mask) for i in range(count)])


SMALL = pltpu.CompilerParams(vmem_limit_bytes=16 * 1024 * 1024)
VM = pl.BlockSpec(memory_space=pltpu.VMEM)
HB = pl.BlockSpec(memory_space=pltpu.HBM)


def body(samples, labels, weights, hist_s, hist_y, counter):
    count, feats = samples.shape
    samp, hist, wrow, part = pl.pallas_call(
        first_kernel,
        in_specs=[HB, HB, HB, HB],
        out_specs=[VM, VM, VM, VM],
        out_shape=[
            pltpu.VMEM((count, feats), bf16),
            pltpu.VMEM((2 * HIST, feats), f32),
            pltpu.VMEM((1, feats), f32),
            pltpu.VMEM((16, 8, 128), f32),
        ],
        scratch_shapes=[pltpu.SemaphoreType.DMA((3 + CHUNKS,))],
        compiler_params=SMALL,
        name="first",
    )(*(pltpu.with_memory_space_constraint(a, pltpu.HBM) for a in (samples, weights.reshape(1, feats), hist_s, hist_y)))
    parts = lax.all_to_all(part, COLS, split_axis=0, concat_axis=0, tiled=True)
    total, cross, gram = pl.pallas_call(
        second_kernel,
        in_specs=[VM] * 5,
        out_specs=[VM] * 3,
        out_shape=[
            pltpu.VMEM((1, feats), f32),
            pltpu.VMEM((128, 1, 128), f32),
            pltpu.VMEM((8, 128), f32),
        ],
        compiler_params=SMALL,
        name="second",
    )(parts, labels.reshape(1, count), samp, hist, wrow)
    crosses = lax.all_to_all(cross, (ROWS, COLS), split_axis=0, concat_axis=0, tiled=True)
    for mask in (7, 3, 1):
        total = swapped(total, mask)
    solve = pl.pallas_call(
        solve_kernel,
        in_specs=[pl.BlockSpec(memory_space=pltpu.SMEM), VM],
        out_specs=VM,
        out_shape=pltpu.VMEM((40, 128), f32),
        compiler_params=SMALL,
        name="solve",
    )(counter, gram)
    new_weights, gradient = pl.pallas_call(
        last_kernel,
        in_specs=[VM] * 5,
        out_specs=[VM] * 2,
        out_shape=[jax.ShapeDtypeStruct((1, feats), f32)] * 2,
        compiler_params=SMALL,
        name="last",
    )(crosses, solve, total, wrow, hist)
    return new_weights.reshape(feats), gradient.reshape(feats)


def solution(mesh):
    return jax.shard_map(
        body,
        mesh=mesh,
        in_specs=(P(ROWS, COLS), P(ROWS), P(COLS), P(None, COLS), P(None, COLS), P()),
        out_specs=(P(COLS), P(COLS)),
        check_vma=False,
    )
```

```python
import jax
import jax.numpy as jnp
from jax import lax
from jax.experimental import pallas as pl
from jax.experimental.pallas import tpu as pltpu
from jax.sharding import PartitionSpec as P


HIST = 16
ROWS = "rows"
COLS = "cols"
CHUNKS = 8

penalty = 4.0
step_length = 0.5
f32 = jnp.float32
bf16 = jnp.bfloat16
highest = lax.Precision.HIGHEST


def iota(shape, axis):
    return lax.broadcasted_iota(jnp.int32, shape, axis)


def dot_t(left, right):
    return lax.dot_general(left, right, (((1,), (1,)), ((), ())), preferred_element_type=f32)


def first_kernel(s_hbm, w_hbm, hs_hbm, hy_hbm, samp, hist, wrow, part, proj, bias, sems):
    feats = samp.shape[1]
    count = samp.shape[0]
    width = feats // CHUNKS
    copies = [
        pltpu.make_async_copy(hs_hbm, hist.at[pl.ds(0, HIST), :], sems.at[0]),
        pltpu.make_async_copy(hy_hbm, hist.at[pl.ds(HIST, HIST), :], sems.at[1]),
        pltpu.make_async_copy(w_hbm, wrow, sems.at[2]),
    ]
    for c in range(CHUNKS):
        cols = pl.ds(c * width, width)
        copies.append(pltpu.make_async_copy(s_hbm.at[:, cols], samp.at[:, cols], sems.at[3 + c]))
    for copy in copies:
        copy.start()
    for copy in copies[:3]:
        copy.wait()
    acc = jnp.zeros((16 + 4 * HIST, count), f32)
    both = jnp.zeros((4 * HIST, 48), f32)
    for c in range(CHUNKS):
        copies[3 + c].wait()
        cols = slice(c * width, (c + 1) * width)
        h = hist[:, cols]
        high = h.astype(bf16)
        low = (h - high.astype(f32)).astype(bf16)
        w = wrow[:, cols]
        w16 = w.astype(bf16)
        w_low = (w - w16.astype(f32)).astype(bf16)
        w_pair = jnp.where(iota((16, width), 0) == 0, w16.astype(f32), w_low.astype(f32)).astype(bf16)
        right = jnp.concatenate([high[HIST:], low[HIST:], w_pair], axis=0)
        left = jnp.concatenate([jnp.broadcast_to(w16, (16, width)), high, low], axis=0)
        acc = acc + dot_t(left, samp[:, cols])
        both = both + dot_t(left[16:], right)
    proj[...] = penalty * (acc[16 : 16 + 2 * HIST] + acc[16 + 2 * HIST :])
    both = jnp.concatenate([both, jnp.zeros((4 * HIST, 80), f32)], axis=1)
    halves = both[: 2 * HIST] + both[2 * HIST :]
    lane = iota((2 * HIST, 128), 1)
    bias[...] = jnp.where(jnp.logical_or(lane == 32, lane == 33), 0.125 * halves, 0.0)
    gram = jnp.where(lane < HIST, halves + pltpu.roll(halves, 128 - HIST, 1), 0.0)
    for shift in (16, 32, 64):
        gram = gram + pltpu.roll(gram, shift, 1)
    gram = jnp.where(lane // HIST == iota((2 * HIST, 128), 0) % 8, gram, 0.0)
    packed = [jnp.sum(gram[8 * a : 8 * a + 8], axis=0, keepdims=True) for a in range(4)]
    rows = [acc[0:1, 128 * i : 128 * i + 128] for i in range(4)]
    mine = jnp.concatenate(rows + packed, axis=0)
    part[...] = jnp.broadcast_to(mine[None], part.shape)


def second_kernel(parts, labels, proj, bias, samp, cross_hbm, gram, total, cross, sem):
    summed = jnp.sum(parts[...], axis=0)
    gram[...] = summed
    margin = jnp.concatenate([summed[i : i + 1] for i in range(4)], axis=1)
    resid = (jax.nn.sigmoid(margin) - labels[...].astype(f32)).astype(bf16)
    prod = proj[...] * resid.astype(f32)
    acc = bias[...]
    for i in range(4):
        acc = acc + prod[:, 128 * i : 128 * i + 128]
    square = jnp.concatenate([acc, jnp.zeros((96, 128), f32)], axis=0)
    line = jnp.sum(square.T, axis=0, keepdims=True)
    cross[...] = jnp.broadcast_to(line[None], cross.shape)
    out = pltpu.make_async_copy(cross, cross_hbm, sem)
    out.start()
    resid16 = jnp.broadcast_to(resid, (16, resid.shape[1]))
    total[...] = jnp.dot(resid16, samp[...], preferred_element_type=f32)[0:1]
    out.wait()


def solve_kernel(counter, gram, out):
    newest = lax.rem(counter[0], HIST)
    row = iota((HIST, 128), 0)
    lane = iota((HIST, 128), 1)
    low_lane = lane < HIST

    def unpacked(a):
        kept = jnp.where(iota((8, 128), 1) // HIST == iota((8, 128), 0), gram[4 + a : 5 + a, :], 0.0)
        for shift in (16, 32, 64):
            kept = kept + pltpu.roll(kept, shift, 1)
        return kept

    sy = jnp.where(low_lane, jnp.concatenate([unpacked(0), unpacked(1)], axis=0), 0.0)
    yy = jnp.where(low_lane, jnp.concatenate([unpacked(2), unpacked(3)], axis=0), 0.0)
    diag = row == lane
    is_new = jnp.logical_and(diag, row == newest)
    pick = lambda m: jnp.sum(jnp.sum(jnp.where(is_new, m, 0.0), axis=0, keepdims=True), axis=1, keepdims=True)
    gamma = pick(sy) / pick(yy)
    rank = lax.rem(newest - row + HIST, HIST)
    curv = jnp.sum(jnp.where(diag, sy, 0.0), axis=1, keepdims=True)
    rho = 1.0 / curv
    inv = diag.astype(f32)
    for step in range(HIST):
        here = row == lax.rem(newest - step + HIST, HIST)
        there = lane == lax.rem(newest - step + HIST, HIST)
        line = jnp.sum(jnp.where(here, inv * rho, 0.0), axis=0, keepdims=True)
        column = jnp.sum(jnp.where(there, sy, 0.0), axis=1, keepdims=True)
        later = inv - column * line
        inv = jnp.where(here, jnp.broadcast_to(line, inv.shape), jnp.where(rank > step, later, inv))
    pad = jnp.zeros((128 - HIST, 128), f32)
    inv_t = jnp.concatenate([inv, pad], axis=0).T[:HIST]
    middle = gamma * yy + jnp.where(diag, sy, 0.0)
    inner = jnp.dot(middle, jnp.concatenate([inv, pad], axis=0), precision=highest, preferred_element_type=f32)
    corner = jnp.dot(inv_t, jnp.concatenate([inner, pad], axis=0), precision=highest, preferred_element_type=f32)
    out[0:HIST, :] = corner - gamma * pltpu.roll(inv_t, HIST, 1)
    out[HIST : 2 * HIST, :] = -gamma * inv
    out[2 * HIST :, :] = jnp.broadcast_to(gamma, (8, 128))


def gradient_kernel(mine, other, solve, wrow, gradient, base):
    weights = wrow[...]
    grad = weights + penalty * (mine[...] + other[...])
    gradient[...] = grad
    base[...] = weights - (step_length * solve[2 * HIST : 2 * HIST + 1, 0:1]) * grad


def last_kernel(crosses, solve, base, hist, new_weights):
    line = jnp.sum(crosses[...], axis=0)
    coefs = step_length * jnp.sum(solve[0 : 2 * HIST, :] * line, axis=1, keepdims=True)
    new_weights[...] = base[...] - jnp.sum(hist[...] * coefs, axis=0, keepdims=True)


def swapped(array, mask):
    count = lax.axis_size(ROWS)
    return lax.ppermute(array, ROWS, [(i, i ^ mask) for i in range(count)])


SMALL = pltpu.CompilerParams(vmem_limit_bytes=16 * 1024 * 1024)
VM = pl.BlockSpec(memory_space=pltpu.VMEM)
HB = pl.BlockSpec(memory_space=pltpu.HBM)


def body(samples, labels, weights, hist_s, hist_y, counter):
    count, feats = samples.shape
    samp, hist, wrow, part, proj, bias = pl.pallas_call(
        first_kernel,
        in_specs=[HB] * 4,
        out_specs=[VM] * 6,
        out_shape=[
            pltpu.VMEM((count, feats), bf16),
            pltpu.VMEM((2 * HIST, feats), f32),
            pltpu.VMEM((1, feats), f32),
            pltpu.VMEM((16, 8, 128), f32),
            pltpu.VMEM((2 * HIST, count), f32),
            pltpu.VMEM((2 * HIST, 128), f32),
        ],
        scratch_shapes=[pltpu.SemaphoreType.DMA((3 + CHUNKS,))],
        compiler_params=SMALL,
        name="first",
    )(*(pltpu.with_memory_space_constraint(a, pltpu.HBM) for a in (samples, weights.reshape(1, feats), hist_s, hist_y)))
    parts = lax.all_to_all(part, COLS, split_axis=0, concat_axis=0, tiled=True)
    cross, gram, total = pl.pallas_call(
        second_kernel,
        in_specs=[VM] * 5,
        out_specs=[HB, VM, VM],
        out_shape=[
            jax.ShapeDtypeStruct((128, 1, 128), f32),
            pltpu.VMEM((8, 128), f32),
            pltpu.VMEM((1, feats), f32),
        ],
        scratch_shapes=[pltpu.VMEM((128, 1, 128), f32), pltpu.SemaphoreType.DMA],
        compiler_params=SMALL,
        name="second",
    )(parts, labels.reshape(1, count), proj, bias, samp)
    crosses = lax.all_to_all(cross, (ROWS, COLS), split_axis=0, concat_axis=0, tiled=True)
    other = swapped(total, 7)
    total = total + other
    other = swapped(total, 3)
    total = total + other
    other = swapped(total, 1)
    solve = pl.pallas_call(
        solve_kernel,
        in_specs=[pl.BlockSpec(memory_space=pltpu.SMEM), VM],
        out_specs=VM,
        out_shape=pltpu.VMEM((40, 128), f32),
        compiler_params=SMALL,
        name="solve",
    )(counter, gram)
    gradient, base = pl.pallas_call(
        gradient_kernel,
        in_specs=[VM] * 4,
        out_specs=[VM] * 2,
        out_shape=[jax.ShapeDtypeStruct((1, feats), f32), pltpu.VMEM((1, feats), f32)],
        compiler_params=SMALL,
        name="gradient",
    )(total, other, solve, wrow)
    new_weights = pl.pallas_call(
        last_kernel,
        in_specs=[VM] * 4,
        out_specs=VM,
        out_shape=jax.ShapeDtypeStruct((1, feats), f32),
        compiler_params=SMALL,
        name="last",
    )(crosses, solve, base, hist)
    return new_weights.reshape(feats), gradient.reshape(feats)


def solution(mesh):
    return jax.shard_map(
        body,
        mesh=mesh,
        in_specs=(P(ROWS, COLS), P(ROWS), P(COLS), P(None, COLS), P(None, COLS), P()),
        out_specs=(P(COLS), P(COLS)),
        check_vma=False,
    )
```

```python
import jax
import jax.numpy as jnp
from jax import lax
from jax.experimental import pallas as pl
from jax.experimental.pallas import tpu as pltpu
from jax.sharding import PartitionSpec as P


HIST = 16
ROWS = "rows"
COLS = "cols"
CHUNKS = 8

penalty = 4.0
step_length = 0.5
f32 = jnp.float32
bf16 = jnp.bfloat16
highest = lax.Precision.HIGHEST


def iota(shape, axis):
    return lax.broadcasted_iota(jnp.int32, shape, axis)


def dot_t(left, right):
    return lax.dot_general(left, right, (((1,), (1,)), ((), ())), preferred_element_type=f32)


def first_kernel(s_hbm, w_hbm, hs_hbm, hy_hbm, samp, hist, wrow, part, sems):
    feats = samp.shape[1]
    width = feats // CHUNKS
    copies = [
        pltpu.make_async_copy(hs_hbm, hist.at[pl.ds(0, HIST), :], sems.at[0]),
        pltpu.make_async_copy(hy_hbm, hist.at[pl.ds(HIST, HIST), :], sems.at[1]),
        pltpu.make_async_copy(w_hbm, wrow, sems.at[2]),
    ]
    for c in range(CHUNKS):
        cols = pl.ds(c * width, width)
        copies.append(pltpu.make_async_copy(s_hbm.at[:, cols], samp.at[:, cols], sems.at[3 + c]))
    for copy in copies:
        copy.start()
    for copy in copies[:3]:
        copy.wait()
    acc = jnp.zeros((16, samp.shape[0]), f32)
    both = jnp.zeros((4 * HIST, 2 * HIST), f32)
    for c in range(CHUNKS):
        copies[3 + c].wait()
        cols = slice(c * width, (c + 1) * width)
        h = hist[:, cols]
        high = h.astype(bf16)
        low = (h - high.astype(f32)).astype(bf16)
        left = jnp.concatenate([high, low], axis=0)
        right = jnp.concatenate([high[HIST:], low[HIST:]], axis=0)
        both = both + dot_t(left, right)
        w16 = jnp.broadcast_to(wrow[:, cols].astype(bf16), (16, width))
        acc = acc + dot_t(w16, samp[:, cols])
    both = jnp.concatenate([both, jnp.zeros((4 * HIST, 128 - 2 * HIST), f32)], axis=1)
    halves = both[: 2 * HIST] + both[2 * HIST :]
    lane = iota((2 * HIST, 128), 1)
    gram = jnp.where(lane < HIST, halves + pltpu.roll(halves, 128 - HIST, 1), 0.0)
    for shift in (16, 32, 64):
        gram = gram + pltpu.roll(gram, shift, 1)
    gram = jnp.where(lane // HIST == iota((2 * HIST, 128), 0) % 8, gram, 0.0)
    packed = [jnp.sum(gram[8 * a : 8 * a + 8], axis=0, keepdims=True) for a in range(4)]
    rows = [acc[0:1, 128 * i : 128 * i + 128] for i in range(4)]
    mine = jnp.concatenate(rows + packed, axis=0)
    part[...] = jnp.broadcast_to(mine[None], part.shape)


def second_kernel(parts, labels, samp, hist, wrow, cross_hbm, gram, total, cross, sem):
    summed = jnp.sum(parts[...], axis=0)
    gram[...] = summed
    margin = jnp.concatenate([summed[i : i + 1] for i in range(4)], axis=1)
    resid = (jax.nn.sigmoid(margin) - labels[...].astype(f32)).astype(bf16)
    resid16 = jnp.broadcast_to(resid, (16, resid.shape[1]))
    width = samp.shape[1] // CHUNKS
    acc = jnp.zeros((2 * HIST, 128), f32)
    for c in range(CHUNKS):
        cols = slice(c * width, (c + 1) * width)
        t = jnp.dot(resid16, samp[:, cols], preferred_element_type=f32)[0:1]
        total[:, cols] = t
        lead = wrow[:, cols] * 0.125 + penalty * t
        prod = hist[:, cols] * lead
        for k in range(width // 128):
            acc = acc + prod[:, 128 * k : 128 * k + 128]
    square = jnp.concatenate([acc, jnp.zeros((128 - 2 * HIST, 128), f32)], axis=0)
    line = jnp.sum(square.T, axis=0, keepdims=True)
    cross[...] = jnp.broadcast_to(line[None], cross.shape)
    out = pltpu.make_async_copy(cross, cross_hbm, sem)
    out.start()
    out.wait()


def solve_kernel(counter, gram, out):
    newest = lax.rem(counter[0], HIST)
    row = iota((HIST, 128), 0)
    lane = iota((HIST, 128), 1)
    low_lane = lane < HIST

    def unpacked(a):
        kept = jnp.where(iota((8, 128), 1) // HIST == iota((8, 128), 0), gram[4 + a : 5 + a, :], 0.0)
        for shift in (16, 32, 64):
            kept = kept + pltpu.roll(kept, shift, 1)
        return kept

    sy = jnp.where(low_lane, jnp.concatenate([unpacked(0), unpacked(1)], axis=0), 0.0)
    yy = jnp.where(low_lane, jnp.concatenate([unpacked(2), unpacked(3)], axis=0), 0.0)
    diag = row == lane
    is_new = jnp.logical_and(diag, row == newest)
    pick = lambda m: jnp.sum(jnp.sum(jnp.where(is_new, m, 0.0), axis=0, keepdims=True), axis=1, keepdims=True)
    gamma = pick(sy) / pick(yy)
    rank = lax.rem(newest - row + HIST, HIST)
    curv = jnp.sum(jnp.where(diag, sy, 0.0), axis=1, keepdims=True)
    rho = 1.0 / curv
    inv = diag.astype(f32)
    for step in range(HIST):
        here = row == lax.rem(newest - step + HIST, HIST)
        there = lane == lax.rem(newest - step + HIST, HIST)
        line = jnp.sum(jnp.where(here, inv * rho, 0.0), axis=0, keepdims=True)
        column = jnp.sum(jnp.where(there, sy, 0.0), axis=1, keepdims=True)
        later = inv - column * line
        inv = jnp.where(here, jnp.broadcast_to(line, inv.shape), jnp.where(rank > step, later, inv))
    pad = jnp.zeros((128 - HIST, 128), f32)
    inv_t = jnp.concatenate([inv, pad], axis=0).T[:HIST]
    middle = gamma * yy + jnp.where(diag, sy, 0.0)
    inner = jnp.dot(middle, jnp.concatenate([inv, pad], axis=0), precision=highest, preferred_element_type=f32)
    corner = jnp.dot(inv_t, jnp.concatenate([inner, pad], axis=0), precision=highest, preferred_element_type=f32)
    out[0:HIST, :] = corner - gamma * pltpu.roll(inv_t, HIST, 1)
    out[HIST : 2 * HIST, :] = -gamma * inv
    out[2 * HIST :, :] = jnp.broadcast_to(gamma, (8, 128))


def gradient_kernel(mine, other, solve, wrow, gradient, base):
    weights = wrow[...]
    grad = weights + penalty * (mine[...] + other[...])
    gradient[...] = grad
    base[...] = weights - (step_length * solve[2 * HIST : 2 * HIST + 1, 0:1]) * grad


def last_kernel(crosses, solve, base, hist, new_weights):
    line = jnp.sum(crosses[...], axis=0)
    coefs = step_length * jnp.sum(solve[0 : 2 * HIST, :] * line, axis=1, keepdims=True)
    new_weights[...] = base[...] - jnp.sum(hist[...] * coefs, axis=0, keepdims=True)


def swapped(array, mask):
    count = lax.axis_size(ROWS)
    return lax.ppermute(array, ROWS, [(i, i ^ mask) for i in range(count)])


SMALL = pltpu.CompilerParams(vmem_limit_bytes=16 * 1024 * 1024)
VM = pl.BlockSpec(memory_space=pltpu.VMEM)
HB = pl.BlockSpec(memory_space=pltpu.HBM)


def body(samples, labels, weights, hist_s, hist_y, counter):
    count, feats = samples.shape
    samp, hist, wrow, part = pl.pallas_call(
        first_kernel,
        in_specs=[HB] * 4,
        out_specs=[VM] * 4,
        out_shape=[
            pltpu.VMEM((count, feats), bf16),
            pltpu.VMEM((2 * HIST, feats), f32),
            pltpu.VMEM((1, feats), f32),
            pltpu.VMEM((16, 8, 128), f32),
        ],
        scratch_shapes=[pltpu.SemaphoreType.DMA((3 + CHUNKS,))],
        compiler_params=SMALL,
        name="first",
    )(*(pltpu.with_memory_space_constraint(a, pltpu.HBM) for a in (samples, weights.reshape(1, feats), hist_s, hist_y)))
    parts = lax.all_to_all(part, COLS, split_axis=0, concat_axis=0, tiled=True)
    cross, gram, total = pl.pallas_call(
        second_kernel,
        in_specs=[VM] * 5,
        out_specs=[HB, VM, VM],
        out_shape=[
            jax.ShapeDtypeStruct((128, 1, 128), f32),
            pltpu.VMEM((8, 128), f32),
            pltpu.VMEM((1, feats), f32),
        ],
        scratch_shapes=[pltpu.VMEM((128, 1, 128), f32), pltpu.SemaphoreType.DMA],
        compiler_params=SMALL,
        name="second",
    )(parts, labels.reshape(1, count), samp, hist, wrow)
    crosses = lax.all_to_all(cross, (ROWS, COLS), split_axis=0, concat_axis=0, tiled=True)
    other = swapped(total, 7)
    total = total + other
    other = swapped(total, 3)
    total = total + other
    other = swapped(total, 1)
    solve = pl.pallas_call(
        solve_kernel,
        in_specs=[pl.BlockSpec(memory_space=pltpu.SMEM), VM],
        out_specs=VM,
        out_shape=pltpu.VMEM((40, 128), f32),
        compiler_params=SMALL,
        name="solve",
    )(counter, gram)
    gradient, base = pl.pallas_call(
        gradient_kernel,
        in_specs=[VM] * 4,
        out_specs=[VM] * 2,
        out_shape=[jax.ShapeDtypeStruct((1, feats), f32), pltpu.VMEM((1, feats), f32)],
        compiler_params=SMALL,
        name="gradient",
    )(total, other, solve, wrow)
    new_weights = pl.pallas_call(
        last_kernel,
        in_specs=[VM] * 4,
        out_specs=VM,
        out_shape=jax.ShapeDtypeStruct((1, feats), f32),
        compiler_params=SMALL,
        name="last",
    )(crosses, solve, base, hist)
    return new_weights.reshape(feats), gradient.reshape(feats)


def solution(mesh):
    return jax.shard_map(
        body,
        mesh=mesh,
        in_specs=(P(ROWS, COLS), P(ROWS), P(COLS), P(None, COLS), P(None, COLS), P()),
        out_specs=(P(COLS), P(COLS)),
        check_vma=False,
    )
```

```python
import jax
import jax.numpy as jnp
from jax import lax
from jax.experimental import pallas as pl
from jax.experimental.pallas import tpu as pltpu
from jax.sharding import PartitionSpec as P


HIST = 16
ROWS = "rows"
COLS = "cols"
CHUNKS = 8

penalty = 4.0
step_length = 0.5
f32 = jnp.float32
bf16 = jnp.bfloat16
highest = lax.Precision.HIGHEST


def iota(shape, axis):
    return lax.broadcasted_iota(jnp.int32, shape, axis)


def dot_t(left, right):
    return lax.dot_general(left, right, (((1,), (1,)), ((), ())), preferred_element_type=f32)


def gram_of(hist):
    h = hist[...]
    high = h.astype(bf16)
    low = (h - high.astype(f32)).astype(bf16)
    both = dot_t(jnp.concatenate([high, low], axis=0), jnp.concatenate([high[HIST:], low[HIST:]], axis=0))
    both = jnp.concatenate([both, jnp.zeros((4 * HIST, 128 - 2 * HIST), f32)], axis=1)
    halves = both[: 2 * HIST] + both[2 * HIST :]
    lane = iota((2 * HIST, 128), 1)
    gram = jnp.where(lane < HIST, halves + pltpu.roll(halves, 128 - HIST, 1), 0.0)
    for shift in (16, 32, 64):
        gram = gram + pltpu.roll(gram, shift, 1)
    gram = jnp.where(lane // HIST == iota((2 * HIST, 128), 0) % 8, gram, 0.0)
    return jnp.concatenate([jnp.sum(gram[8 * a : 8 * a + 8], axis=0, keepdims=True) for a in range(4)], axis=0)


def first_kernel(s_hbm, w_hbm, hs_hbm, hy_hbm, samp, hist, wrow, part, sems):
    feats = samp.shape[1]
    width = feats // CHUNKS
    copies = [pltpu.make_async_copy(w_hbm, wrow, sems.at[0])]
    for c in range(CHUNKS):
        cols = pl.ds(c * width, width)
        copies.append(pltpu.make_async_copy(s_hbm.at[:, cols], samp.at[:, cols], sems.at[1 + c]))
    copies.append(pltpu.make_async_copy(hs_hbm, hist.at[pl.ds(0, HIST), :], sems.at[1 + CHUNKS]))
    copies.append(pltpu.make_async_copy(hy_hbm, hist.at[pl.ds(HIST, HIST), :], sems.at[2 + CHUNKS]))
    for copy in copies:
        copy.start()
    copies[0].wait()
    acc = jnp.zeros((16, samp.shape[0]), f32)
    for c in range(CHUNKS):
        copies[1 + c].wait()
        cols = slice(c * width, (c + 1) * width)
        w16 = jnp.broadcast_to(wrow[:, cols].astype(bf16), (16, width))
        acc = acc + dot_t(w16, samp[:, cols])
    rows = [acc[0:1, 128 * i : 128 * i + 128] for i in range(4)]
    mine = jnp.concatenate(rows + [jnp.zeros((4, 128), f32)], axis=0)
    part[...] = jnp.broadcast_to(mine[None], part.shape)
    copies[1 + CHUNKS].wait()
    copies[2 + CHUNKS].wait()

    @pl.when(lax.axis_index(ROWS) % 2 == 1)
    def _():
        part[:, 4:8, :] = jnp.broadcast_to(gram_of(hist)[None], (part.shape[0], 4, 128))


def second_kernel(parts, labels, samp, hist, wrow, cross_hbm, total, cross, sem):
    summed = jnp.sum(parts[...], axis=0)
    feats = samp.shape[1]
    for i in range(4):
        total[:, feats + 128 * i : feats + 128 * i + 128] = summed[4 + i : 5 + i]
    margin = jnp.concatenate([summed[i : i + 1] for i in range(4)], axis=1)
    resid = (jax.nn.sigmoid(margin) - labels[...].astype(f32)).astype(bf16)
    resid16 = jnp.broadcast_to(resid, (16, resid.shape[1]))
    width = feats // CHUNKS
    acc = jnp.zeros((2 * HIST, 128), f32)
    for c in range(CHUNKS):
        cols = slice(c * width, (c + 1) * width)
        t = jnp.dot(resid16, samp[:, cols], preferred_element_type=f32)[0:1]
        total[:, cols] = t
        lead = wrow[:, cols] * 0.125 + penalty * t
        prod = hist[:, cols] * lead
        for k in range(width // 128):
            acc = acc + prod[:, 128 * k : 128 * k + 128]
    square = jnp.concatenate([acc, jnp.zeros((128 - 2 * HIST, 128), f32)], axis=0)
    line = jnp.sum(square.T, axis=0, keepdims=True)
    cross[...] = jnp.broadcast_to(line[None], cross.shape)
    out = pltpu.make_async_copy(cross, cross_hbm, sem)
    out.start()
    out.wait()


def solve_kernel(counter, gram, out):
    newest = lax.rem(counter[0], HIST)
    row = iota((HIST, 128), 0)
    lane = iota((HIST, 128), 1)
    low_lane = lane < HIST

    def unpacked(a):
        kept = jnp.where(iota((8, 128), 1) // HIST == iota((8, 128), 0), gram[:, 128 * a : 128 * a + 128], 0.0)
        for shift in (16, 32, 64):
            kept = kept + pltpu.roll(kept, shift, 1)
        return kept

    sy = jnp.where(low_lane, jnp.concatenate([unpacked(0), unpacked(1)], axis=0), 0.0)
    yy = jnp.where(low_lane, jnp.concatenate([unpacked(2), unpacked(3)], axis=0), 0.0)
    diag = row == lane
    is_new = jnp.logical_and(diag, row == newest)
    pick = lambda m: jnp.sum(jnp.sum(jnp.where(is_new, m, 0.0), axis=0, keepdims=True), axis=1, keepdims=True)
    gamma = pick(sy) / pick(yy)
    rank = lax.rem(newest - row + HIST, HIST)
    curv = jnp.sum(jnp.where(diag, sy, 0.0), axis=1, keepdims=True)
    rho = 1.0 / curv
    inv = diag.astype(f32)
    for step in range(HIST):
        here = row == lax.rem(newest - step + HIST, HIST)
        there = lane == lax.rem(newest - step + HIST, HIST)
        line = jnp.sum(jnp.where(here, inv * rho, 0.0), axis=0, keepdims=True)
        column = jnp.sum(jnp.where(there, sy, 0.0), axis=1, keepdims=True)
        later = inv - column * line
        inv = jnp.where(here, jnp.broadcast_to(line, inv.shape), jnp.where(rank > step, later, inv))
    pad = jnp.zeros((128 - HIST, 128), f32)
    inv_t = jnp.concatenate([inv, pad], axis=0).T[:HIST]
    middle = gamma * yy + jnp.where(diag, sy, 0.0)
    inner = jnp.dot(middle, jnp.concatenate([inv, pad], axis=0), precision=highest, preferred_element_type=f32)
    corner = jnp.dot(inv_t, jnp.concatenate([inner, pad], axis=0), precision=highest, preferred_element_type=f32)
    out[0:HIST, :] = corner - gamma * pltpu.roll(inv_t, HIST, 1)
    out[HIST : 2 * HIST, :] = -gamma * inv
    out[2 * HIST :, :] = jnp.broadcast_to(gamma, (8, 128))


def gradient_kernel(mine, other, solve, wrow, gradient, base):
    weights = wrow[...]
    grad = weights + penalty * (mine[...] + other[...])
    gradient[...] = grad
    base[...] = weights - (step_length * solve[2 * HIST : 2 * HIST + 1, 0:1]) * grad


def last_kernel(crosses, solve, base, hist, new_weights):
    line = jnp.sum(crosses[...], axis=0)
    coefs = step_length * jnp.sum(solve[0 : 2 * HIST, :] * line, axis=1, keepdims=True)
    new_weights[...] = base[...] - jnp.sum(hist[...] * coefs, axis=0, keepdims=True)


def swapped(array, mask):
    count = lax.axis_size(ROWS)
    return lax.ppermute(array, ROWS, [(i, i ^ mask) for i in range(count)])


SMALL = pltpu.CompilerParams(vmem_limit_bytes=16 * 1024 * 1024)
VM = pl.BlockSpec(memory_space=pltpu.VMEM)
HB = pl.BlockSpec(memory_space=pltpu.HBM)


def body(samples, labels, weights, hist_s, hist_y, counter):
    count, feats = samples.shape
    samp, hist, wrow, part = pl.pallas_call(
        first_kernel,
        in_specs=[HB] * 4,
        out_specs=[VM] * 4,
        out_shape=[
            pltpu.VMEM((count, feats), bf16),
            pltpu.VMEM((2 * HIST, feats), f32),
            pltpu.VMEM((1, feats), f32),
            pltpu.VMEM((16, 8, 128), f32),
        ],
        scratch_shapes=[pltpu.SemaphoreType.DMA((3 + CHUNKS,))],
        compiler_params=SMALL,
        name="first",
    )(*(pltpu.with_memory_space_constraint(a, pltpu.HBM) for a in (samples, weights.reshape(1, feats), hist_s, hist_y)))
    parts = lax.all_to_all(part, COLS, split_axis=0, concat_axis=0, tiled=True)
    cross, total = pl.pallas_call(
        second_kernel,
        in_specs=[VM] * 5,
        out_specs=[HB, VM],
        out_shape=[
            jax.ShapeDtypeStruct((128, 1, 128), f32),
            pltpu.VMEM((1, feats + 512), f32),
        ],
        scratch_shapes=[pltpu.VMEM((128, 1, 128), f32), pltpu.SemaphoreType.DMA],
        compiler_params=SMALL,
        name="second",
    )(parts, labels.reshape(1, count), samp, hist, wrow)
    crosses = lax.all_to_all(cross, (ROWS, COLS), split_axis=0, concat_axis=0, tiled=True)
    other = swapped(total, 1)
    total = total + other
    gram = total[:, feats:]
    total = total[:, :feats]
    other = swapped(total, 3)
    total = total + other
    other = swapped(total, 7)
    solve = pl.pallas_call(
        solve_kernel,
        in_specs=[pl.BlockSpec(memory_space=pltpu.SMEM), VM],
        out_specs=VM,
        out_shape=pltpu.VMEM((40, 128), f32),
        compiler_params=SMALL,
        name="solve",
    )(counter, gram)
    gradient, base = pl.pallas_call(
        gradient_kernel,
        in_specs=[VM] * 4,
        out_specs=[VM] * 2,
        out_shape=[pltpu.VMEM((1, feats), f32), pltpu.VMEM((1, feats), f32)],
        compiler_params=SMALL,
        name="gradient",
    )(total, other, solve, wrow)
    new_weights = pl.pallas_call(
        last_kernel,
        in_specs=[VM] * 4,
        out_specs=VM,
        out_shape=jax.ShapeDtypeStruct((1, feats), f32),
        compiler_params=SMALL,
        name="last",
    )(crosses, solve, base, hist)
    return new_weights.reshape(feats), gradient.reshape(feats)


def solution(mesh):
    return jax.shard_map(
        body,
        mesh=mesh,
        in_specs=(P(ROWS, COLS), P(ROWS), P(COLS), P(None, COLS), P(None, COLS), P()),
        out_specs=(P(COLS), P(COLS)),
        check_vma=False,
    )
```

```python
import jax
import jax.numpy as jnp
from jax import lax
from jax.experimental import pallas as pl
from jax.experimental.pallas import tpu as pltpu
from jax.sharding import PartitionSpec as P


HIST = 16
ROWS = "rows"
COLS = "cols"
CHUNKS = 8

penalty = 4.0
step_length = 0.5
f32 = jnp.float32
bf16 = jnp.bfloat16
highest = lax.Precision.HIGHEST


def iota(shape, axis):
    return lax.broadcasted_iota(jnp.int32, shape, axis)


def dot_t(left, right):
    return lax.dot_general(left, right, (((1,), (1,)), ((), ())), preferred_element_type=f32)


def gram_of(hist):
    h = hist[...]
    high = h.astype(bf16)
    low = (h - high.astype(f32)).astype(bf16)
    both = dot_t(jnp.concatenate([high, low], axis=0), jnp.concatenate([high[HIST:], low[HIST:]], axis=0))
    both = jnp.concatenate([both, jnp.zeros((4 * HIST, 128 - 2 * HIST), f32)], axis=1)
    halves = both[: 2 * HIST] + both[2 * HIST :]
    lane = iota((2 * HIST, 128), 1)
    gram = jnp.where(lane < HIST, halves + pltpu.roll(halves, 128 - HIST, 1), 0.0)
    for shift in (16, 32, 64):
        gram = gram + pltpu.roll(gram, shift, 1)
    gram = jnp.where(lane // HIST == iota((2 * HIST, 128), 0) % 8, gram, 0.0)
    return jnp.concatenate([jnp.sum(gram[8 * a : 8 * a + 8], axis=0, keepdims=True) for a in range(4)], axis=0)


def first_kernel(s_hbm, w_hbm, hs_hbm, hy_hbm, samp, hist, wrow, part, sems):
    feats = samp.shape[1]
    width = feats // CHUNKS
    copies = [pltpu.make_async_copy(w_hbm, wrow, sems.at[0])]
    for c in range(CHUNKS):
        cols = pl.ds(c * width, width)
        copies.append(pltpu.make_async_copy(s_hbm.at[:, cols], samp.at[:, cols], sems.at[1 + c]))
    copies.append(pltpu.make_async_copy(hs_hbm, hist.at[pl.ds(0, HIST), :], sems.at[1 + CHUNKS]))
    copies.append(pltpu.make_async_copy(hy_hbm, hist.at[pl.ds(HIST, HIST), :], sems.at[2 + CHUNKS]))
    for copy in copies:
        copy.start()
    copies[0].wait()
    acc = jnp.zeros((16, samp.shape[0]), f32)
    for c in range(CHUNKS):
        copies[1 + c].wait()
        cols = slice(c * width, (c + 1) * width)
        w16 = jnp.broadcast_to(wrow[:, cols].astype(bf16), (16, width))
        acc = acc + dot_t(w16, samp[:, cols])
    rows = [acc[0:1, 128 * i : 128 * i + 128] for i in range(4)]
    mine = jnp.concatenate(rows + [jnp.zeros((4, 128), f32)], axis=0)
    part[...] = jnp.broadcast_to(mine[None], part.shape)
    copies[1 + CHUNKS].wait()
    copies[2 + CHUNKS].wait()

    @pl.when(lax.axis_index(ROWS) % 2 == 1)
    def _():
        part[:, 4:8, :] = jnp.broadcast_to(gram_of(hist)[None], (part.shape[0], 4, 128))


def second_kernel(parts, labels, samp, hist, wrow, cross_hbm, total, cross, sem):
    summed = jnp.sum(parts[...], axis=0)
    feats = samp.shape[1]
    for i in range(4):
        total[:, feats + 128 * i : feats + 128 * i + 128] = summed[4 + i : 5 + i]
    margin = jnp.concatenate([summed[i : i + 1] for i in range(4)], axis=1)
    resid = (jax.nn.sigmoid(margin) - labels[...].astype(f32)).astype(bf16)
    resid16 = jnp.broadcast_to(resid, (16, resid.shape[1]))
    width = feats // CHUNKS
    acc = jnp.zeros((2 * HIST, 128), f32)
    for c in range(CHUNKS):
        cols = slice(c * width, (c + 1) * width)
        t = jnp.dot(resid16, samp[:, cols], preferred_element_type=f32)[0:1]
        total[:, cols] = t
        lead = wrow[:, cols] * 0.125 + penalty * t
        prod = hist[:, cols] * lead
        for k in range(width // 128):
            acc = acc + prod[:, 128 * k : 128 * k + 128]
    square = jnp.concatenate([acc, jnp.zeros((128 - 2 * HIST, 128), f32)], axis=0)
    line = jnp.sum(square.T, axis=0, keepdims=True)
    cross[...] = jnp.broadcast_to(line[None], cross.shape)
    out = pltpu.make_async_copy(cross, cross_hbm, sem)
    out.start()
    out.wait()


def solve_kernel(counter, gram, out):
    newest = lax.rem(counter[0], HIST)
    row = iota((HIST, 128), 0)
    lane = iota((HIST, 128), 1)
    low_lane = lane < HIST

    def unpacked(a):
        kept = jnp.where(iota((8, 128), 1) // HIST == iota((8, 128), 0), gram[:, 128 * a : 128 * a + 128], 0.0)
        for shift in (16, 32, 64):
            kept = kept + pltpu.roll(kept, shift, 1)
        return kept

    sy = jnp.where(low_lane, jnp.concatenate([unpacked(0), unpacked(1)], axis=0), 0.0)
    yy = jnp.where(low_lane, jnp.concatenate([unpacked(2), unpacked(3)], axis=0), 0.0)
    diag = row == lane
    is_new = jnp.logical_and(diag, row == newest)
    pick = lambda m: jnp.sum(jnp.sum(jnp.where(is_new, m, 0.0), axis=0, keepdims=True), axis=1, keepdims=True)
    gamma = pick(sy) / pick(yy)
    rank = lax.rem(newest - row + HIST, HIST)
    curv = jnp.sum(jnp.where(diag, sy, 0.0), axis=1, keepdims=True)
    rho = 1.0 / curv
    inv = diag.astype(f32)
    for step in range(HIST):
        here = row == lax.rem(newest - step + HIST, HIST)
        there = lane == lax.rem(newest - step + HIST, HIST)
        line = jnp.sum(jnp.where(here, inv * rho, 0.0), axis=0, keepdims=True)
        column = jnp.sum(jnp.where(there, sy, 0.0), axis=1, keepdims=True)
        later = inv - column * line
        inv = jnp.where(here, jnp.broadcast_to(line, inv.shape), jnp.where(rank > step, later, inv))
    pad = jnp.zeros((128 - HIST, 128), f32)
    inv_t = jnp.concatenate([inv, pad], axis=0).T[:HIST]
    middle = gamma * yy + jnp.where(diag, sy, 0.0)
    inner = jnp.dot(middle, jnp.concatenate([inv, pad], axis=0), precision=highest, preferred_element_type=f32)
    corner = jnp.dot(inv_t, jnp.concatenate([inner, pad], axis=0), precision=highest, preferred_element_type=f32)
    out[0:HIST, :] = corner - gamma * pltpu.roll(inv_t, HIST, 1)
    out[HIST : 2 * HIST, :] = -gamma * inv
    out[2 * HIST :, :] = jnp.broadcast_to(gamma, (8, 128))


def gradient_kernel(mine, other, solve, wrow, gradient, base):
    weights = wrow[...]
    grad = weights + penalty * (mine[...] + other[...])
    gradient[...] = grad
    base[...] = weights - (step_length * solve[2 * HIST : 2 * HIST + 1, 0:1]) * grad


def last_kernel(crosses, solve, base, hist, new_weights):
    line = jnp.sum(jnp.sum(crosses[...], axis=0), axis=0, keepdims=True)
    coefs = step_length * jnp.sum(solve[0 : 2 * HIST, :] * line, axis=1, keepdims=True)
    new_weights[...] = base[...] - jnp.sum(hist[...] * coefs, axis=0, keepdims=True)


def swapped(array, mask):
    count = lax.axis_size(ROWS)
    return lax.ppermute(array, ROWS, [(i, i ^ mask) for i in range(count)])


SMALL = pltpu.CompilerParams(vmem_limit_bytes=16 * 1024 * 1024)
VM = pl.BlockSpec(memory_space=pltpu.VMEM)
HB = pl.BlockSpec(memory_space=pltpu.HBM)


def body(samples, labels, weights, hist_s, hist_y, counter):
    count, feats = samples.shape
    samp, hist, wrow, part = pl.pallas_call(
        first_kernel,
        in_specs=[HB] * 4,
        out_specs=[VM] * 4,
        out_shape=[
            pltpu.VMEM((count, feats), bf16),
            pltpu.VMEM((2 * HIST, feats), f32),
            pltpu.VMEM((1, feats), f32),
            pltpu.VMEM((16, 8, 128), f32),
        ],
        scratch_shapes=[pltpu.SemaphoreType.DMA((3 + CHUNKS,))],
        compiler_params=SMALL,
        name="first",
    )(*(pltpu.with_memory_space_constraint(a, pltpu.HBM) for a in (samples, weights.reshape(1, feats), hist_s, hist_y)))
    parts = lax.all_to_all(part, COLS, split_axis=0, concat_axis=0, axis_index_groups=[[15] + [i for i in range(16) if i != 15]], tiled=True)
    cross, total = pl.pallas_call(
        second_kernel,
        in_specs=[VM] * 5,
        out_specs=[HB, VM],
        out_shape=[
            jax.ShapeDtypeStruct((128, 1, 128), f32),
            pltpu.VMEM((1, feats + 512), f32),
        ],
        scratch_shapes=[pltpu.VMEM((128, 1, 128), f32), pltpu.SemaphoreType.DMA],
        compiler_params=SMALL,
        name="second",
    )(parts, labels.reshape(1, count), samp, hist, wrow)
    crosses = lax.all_to_all(cross, (ROWS, COLS), split_axis=0, concat_axis=0, axis_index_groups=[list(range(127, -1, -1))], tiled=True)
    other = swapped(total, 1)
    total = total + other
    gram = total[:, feats:]
    total = total[:, :feats]
    other = swapped(total, 3)
    total = total + other
    other = swapped(total, 7)
    solve = pl.pallas_call(
        solve_kernel,
        in_specs=[pl.BlockSpec(memory_space=pltpu.SMEM), VM],
        out_specs=VM,
        out_shape=pltpu.VMEM((40, 128), f32),
        compiler_params=SMALL,
        name="solve",
    )(counter, gram)
    gradient, base = pl.pallas_call(
        gradient_kernel,
        in_specs=[VM] * 4,
        out_specs=[VM] * 2,
        out_shape=[pltpu.VMEM((1, feats), f32), pltpu.VMEM((1, feats), f32)],
        compiler_params=SMALL,
        name="gradient",
    )(total, other, solve, wrow)
    new_weights = pl.pallas_call(
        last_kernel,
        in_specs=[VM] * 4,
        out_specs=VM,
        out_shape=jax.ShapeDtypeStruct((1, feats), f32),
        compiler_params=SMALL,
        name="last",
    )(crosses.reshape(16, 8, 128), solve, base, hist)
    return new_weights.reshape(feats), gradient.reshape(feats)


def solution(mesh):
    return jax.shard_map(
        body,
        mesh=mesh,
        in_specs=(P(ROWS, COLS), P(ROWS), P(COLS), P(None, COLS), P(None, COLS), P()),
        out_specs=(P(COLS), P(COLS)),
        check_vma=False,
    )
```

```python
import jax
import jax.numpy as jnp
from jax import lax
from jax.experimental import pallas as pl
from jax.experimental.pallas import tpu as pltpu
from jax.sharding import Mesh
from jax.sharding import PartitionSpec as P


HIST = 16
ROWS = ("x", "core")
COLS = "cols"
CHUNKS = 8

penalty = 4.0
step_length = 0.5
f32 = jnp.float32
bf16 = jnp.bfloat16
highest = lax.Precision.HIGHEST


def iota(shape, axis):
    return lax.broadcasted_iota(jnp.int32, shape, axis)


def dot_t(left, right):
    return lax.dot_general(left, right, (((1,), (1,)), ((), ())), preferred_element_type=f32)


def gram_of(hist):
    h = hist[...]
    high = h.astype(bf16)
    low = (h - high.astype(f32)).astype(bf16)
    both = dot_t(jnp.concatenate([high, low], axis=0), jnp.concatenate([high[HIST:], low[HIST:]], axis=0))
    both = jnp.concatenate([both, jnp.zeros((4 * HIST, 128 - 2 * HIST), f32)], axis=1)
    halves = both[: 2 * HIST] + both[2 * HIST :]
    lane = iota((2 * HIST, 128), 1)
    gram = jnp.where(lane < HIST, halves + pltpu.roll(halves, 128 - HIST, 1), 0.0)
    for shift in (16, 32, 64):
        gram = gram + pltpu.roll(gram, shift, 1)
    gram = jnp.where(lane // HIST == iota((2 * HIST, 128), 0) % 8, gram, 0.0)
    return jnp.concatenate([jnp.sum(gram[8 * a : 8 * a + 8], axis=0, keepdims=True) for a in range(4)], axis=0)


def first_kernel(s_hbm, w_hbm, hs_hbm, hy_hbm, samp, hist, wrow, part, sems):
    feats = samp.shape[1]
    width = feats // CHUNKS
    copies = [pltpu.make_async_copy(w_hbm, wrow, sems.at[0])]
    for c in range(CHUNKS):
        cols = pl.ds(c * width, width)
        copies.append(pltpu.make_async_copy(s_hbm.at[:, cols], samp.at[:, cols], sems.at[1 + c]))
    copies.append(pltpu.make_async_copy(hs_hbm, hist.at[pl.ds(0, HIST), :], sems.at[1 + CHUNKS]))
    copies.append(pltpu.make_async_copy(hy_hbm, hist.at[pl.ds(HIST, HIST), :], sems.at[2 + CHUNKS]))
    for copy in copies:
        copy.start()
    copies[0].wait()
    acc = jnp.zeros((16, samp.shape[0]), f32)
    for c in range(CHUNKS):
        copies[1 + c].wait()
        cols = slice(c * width, (c + 1) * width)
        w16 = jnp.broadcast_to(wrow[:, cols].astype(bf16), (16, width))
        acc = acc + dot_t(w16, samp[:, cols])
    rows = [acc[0:1, 128 * i : 128 * i + 128] for i in range(4)]
    mine = jnp.concatenate(rows + [jnp.zeros((4, 128), f32)], axis=0)
    part[...] = jnp.broadcast_to(mine[None], part.shape)
    copies[1 + CHUNKS].wait()
    copies[2 + CHUNKS].wait()

    @pl.when(lax.axis_index("core") == 1)
    def _():
        part[:, 4:8, :] = jnp.broadcast_to(gram_of(hist)[None], (part.shape[0], 4, 128))


def second_kernel(parts, labels, samp, hist, wrow, packed):
    summed = jnp.sum(parts[...], axis=0)
    feats = samp.shape[1]
    for i in range(4):
        packed[:, feats + 128 * i : feats + 128 * i + 128] = summed[4 + i : 5 + i]
    margin = jnp.concatenate([summed[i : i + 1] for i in range(4)], axis=1)
    resid = (jax.nn.sigmoid(margin) - labels[...].astype(f32)).astype(bf16)
    resid16 = jnp.broadcast_to(resid, (16, resid.shape[1]))
    width = feats // CHUNKS
    acc = jnp.zeros((2 * HIST, 128), f32)
    for c in range(CHUNKS):
        cols = slice(c * width, (c + 1) * width)
        t = jnp.dot(resid16, samp[:, cols], preferred_element_type=f32)[0:1]
        packed[:, cols] = t
        lead = wrow[:, cols] * 0.125 + penalty * t
        prod = hist[:, cols] * lead
        for k in range(width // 128):
            acc = acc + prod[:, 128 * k : 128 * k + 128]
    square = jnp.concatenate([acc, jnp.zeros((128 - 2 * HIST, 128), f32)], axis=0)
    packed[:, feats + 512 :] = jnp.sum(square.T, axis=0, keepdims=True)


def spread_kernel(mine, other, cross_hbm, total, gram, cross, sem):
    feats = total.shape[1]
    line = mine[:, feats + 512 :] + other[:, feats + 512 :]
    cross[...] = jnp.broadcast_to(line[None], cross.shape)
    out = pltpu.make_async_copy(cross, cross_hbm, sem)
    out.start()
    total[...] = mine[:, :feats] + other[:, :feats]
    gram[...] = mine[:, feats : feats + 512] + other[:, feats : feats + 512]
    out.wait()


def solve_kernel(counter, gram, out):
    newest = lax.rem(counter[0], HIST)
    row = iota((HIST, 128), 0)
    lane = iota((HIST, 128), 1)
    low_lane = lane < HIST

    def unpacked(a):
        kept = jnp.where(iota((8, 128), 1) // HIST == iota((8, 128), 0), gram[:, 128 * a : 128 * a + 128], 0.0)
        for shift in (16, 32, 64):
            kept = kept + pltpu.roll(kept, shift, 1)
        return kept

    sy = jnp.where(low_lane, jnp.concatenate([unpacked(0), unpacked(1)], axis=0), 0.0)
    yy = jnp.where(low_lane, jnp.concatenate([unpacked(2), unpacked(3)], axis=0), 0.0)
    diag = row == lane
    is_new = jnp.logical_and(diag, row == newest)
    pick = lambda m: jnp.sum(jnp.sum(jnp.where(is_new, m, 0.0), axis=0, keepdims=True), axis=1, keepdims=True)
    gamma = pick(sy) / pick(yy)
    rank = lax.rem(newest - row + HIST, HIST)
    curv = jnp.sum(jnp.where(diag, sy, 0.0), axis=1, keepdims=True)
    rho = 1.0 / curv
    inv = diag.astype(f32)
    for step in range(HIST):
        here = row == lax.rem(newest - step + HIST, HIST)
        there = lane == lax.rem(newest - step + HIST, HIST)
        line = jnp.sum(jnp.where(here, inv * rho, 0.0), axis=0, keepdims=True)
        column = jnp.sum(jnp.where(there, sy, 0.0), axis=1, keepdims=True)
        later = inv - column * line
        inv = jnp.where(here, jnp.broadcast_to(line, inv.shape), jnp.where(rank > step, later, inv))
    pad = jnp.zeros((128 - HIST, 128), f32)
    inv_t = jnp.concatenate([inv, pad], axis=0).T[:HIST]
    middle = gamma * yy + jnp.where(diag, sy, 0.0)
    inner = jnp.dot(middle, jnp.concatenate([inv, pad], axis=0), precision=highest, preferred_element_type=f32)
    corner = jnp.dot(inv_t, jnp.concatenate([inner, pad], axis=0), precision=highest, preferred_element_type=f32)
    out[0:HIST, :] = corner - gamma * pltpu.roll(inv_t, HIST, 1)
    out[HIST : 2 * HIST, :] = -gamma * inv
    out[2 * HIST :, :] = jnp.broadcast_to(gamma, (8, 128))


def last_kernel(crosses, solve, mine, other, wrow, hist, new_weights, gradient):
    line = jnp.sum(jnp.sum(crosses[...], axis=0), axis=0, keepdims=True)
    coefs = step_length * jnp.sum(solve[0 : 2 * HIST, :] * line, axis=1, keepdims=True)
    weights = wrow[...]
    grad = weights + penalty * (mine[...] + other[...])
    gradient[...] = grad
    base = weights - (step_length * solve[2 * HIST : 2 * HIST + 1, 0:1]) * grad
    new_weights[...] = base - jnp.sum(hist[...] * coefs, axis=0, keepdims=True)


def swapped(array, mask):
    count = lax.axis_size(ROWS)
    return lax.ppermute(array, ROWS, [(i, i ^ mask) for i in range(count)])


SMALL = pltpu.CompilerParams(vmem_limit_bytes=16 * 1024 * 1024)
VM = pl.BlockSpec(memory_space=pltpu.VMEM)
HB = pl.BlockSpec(memory_space=pltpu.HBM)


def body(samples, labels, weights, hist_s, hist_y, counter):
    count, feats = samples.shape
    samp, hist, wrow, part = pl.pallas_call(
        first_kernel,
        in_specs=[HB] * 4,
        out_specs=[VM] * 4,
        out_shape=[
            pltpu.VMEM((count, feats), bf16),
            pltpu.VMEM((2 * HIST, feats), f32),
            pltpu.VMEM((1, feats), f32),
            pltpu.VMEM((16, 8, 128), f32),
        ],
        scratch_shapes=[pltpu.SemaphoreType.DMA((3 + CHUNKS,))],
        compiler_params=SMALL,
        name="first",
    )(*(pltpu.with_memory_space_constraint(a, pltpu.HBM) for a in (samples, weights.reshape(1, feats), hist_s, hist_y)))
    parts = lax.all_to_all(part, COLS, split_axis=0, concat_axis=0, axis_index_groups=[[15] + list(range(15))], tiled=True)
    packed = pl.pallas_call(
        second_kernel,
        in_specs=[VM] * 5,
        out_specs=VM,
        out_shape=pltpu.VMEM((1, feats + 640), f32),
        compiler_params=SMALL,
        name="second",
    )(parts, labels.reshape(1, count), samp, hist, wrow)
    other = swapped(packed, 1)
    cross, total, gram = pl.pallas_call(
        spread_kernel,
        in_specs=[VM] * 2,
        out_specs=[HB, VM, VM],
        out_shape=[
            jax.ShapeDtypeStruct((8, 8, 128), f32),
            pltpu.VMEM((1, feats), f32),
            pltpu.VMEM((1, 512), f32),
        ],
        scratch_shapes=[pltpu.VMEM((8, 8, 128), f32), pltpu.SemaphoreType.DMA],
        compiler_params=SMALL,
        name="spread",
    )(packed, other)
    crosses = lax.all_to_all(cross.reshape(64, 1, 128), ("x", COLS), split_axis=0, concat_axis=0, axis_index_groups=[list(range(63, -1, -1))], tiled=True)
    other = swapped(total, 3)
    total = total + other
    other = swapped(total, 6)
    solve = pl.pallas_call(
        solve_kernel,
        in_specs=[pl.BlockSpec(memory_space=pltpu.SMEM), VM],
        out_specs=VM,
        out_shape=pltpu.VMEM((40, 128), f32),
        compiler_params=SMALL,
        name="solve",
    )(counter, gram)
    new_weights, gradient = pl.pallas_call(
        last_kernel,
        in_specs=[VM] * 6,
        out_specs=[VM] * 2,
        out_shape=[jax.ShapeDtypeStruct((1, feats), f32)] * 2,
        compiler_params=SMALL,
        name="last",
    )(crosses.reshape(8, 8, 128), solve, total, other, wrow, hist)
    return new_weights.reshape(feats), gradient.reshape(feats)


def solution(mesh):
    split = Mesh(mesh.devices.reshape(4, 2, 16), ("x", "core", COLS))
    return jax.shard_map(
        body,
        mesh=split,
        in_specs=(P(ROWS, COLS), P(ROWS), P(COLS), P(None, COLS), P(None, COLS), P()),
        out_specs=(P(COLS), P(COLS)),
        check_vma=False,
    )
```

```python
import jax
import jax.numpy as jnp
from jax import lax
from jax.experimental import pallas as pl
from jax.experimental.pallas import tpu as pltpu
from jax.sharding import Mesh
from jax.sharding import PartitionSpec as P


HIST = 16
ROWS = ("x", "core")
COLS = "cols"
CHUNKS = 16

penalty = 4.0
step_length = 0.5
f32 = jnp.float32
bf16 = jnp.bfloat16
highest = lax.Precision.HIGHEST


def iota(shape, axis):
    return lax.broadcasted_iota(jnp.int32, shape, axis)


def dot_t(left, right):
    return lax.dot_general(left, right, (((1,), (1,)), ((), ())), preferred_element_type=f32)


def gram_of(hist):
    h = hist[...]
    high = h.astype(bf16)
    low = (h - high.astype(f32)).astype(bf16)
    both = dot_t(jnp.concatenate([high, low], axis=0), jnp.concatenate([high[HIST:], low[HIST:]], axis=0))
    both = jnp.concatenate([both, jnp.zeros((4 * HIST, 128 - 2 * HIST), f32)], axis=1)
    halves = both[: 2 * HIST] + both[2 * HIST :]
    lane = iota((2 * HIST, 128), 1)
    gram = jnp.where(lane < HIST, halves + pltpu.roll(halves, 128 - HIST, 1), 0.0)
    for shift in (16, 32, 64):
        gram = gram + pltpu.roll(gram, shift, 1)
    gram = jnp.where(lane // HIST == iota((2 * HIST, 128), 0) % 8, gram, 0.0)
    return jnp.concatenate([jnp.sum(gram[8 * a : 8 * a + 8], axis=0, keepdims=True) for a in range(4)], axis=0)


def first_kernel(s_hbm, w_hbm, hs_hbm, hy_hbm, samp, hist, wrow, part, sems):
    feats = samp.shape[1]
    width = feats // CHUNKS
    copies = [pltpu.make_async_copy(w_hbm, wrow, sems.at[0])]
    for c in range(CHUNKS):
        cols = pl.ds(c * width, width)
        copies.append(pltpu.make_async_copy(s_hbm.at[:, cols], samp.at[:, cols], sems.at[1 + c]))
    copies.append(pltpu.make_async_copy(hs_hbm, hist.at[pl.ds(0, HIST), :], sems.at[1 + CHUNKS]))
    copies.append(pltpu.make_async_copy(hy_hbm, hist.at[pl.ds(HIST, HIST), :], sems.at[2 + CHUNKS]))
    for copy in copies:
        copy.start()
    copies[0].wait()
    acc = jnp.zeros((16, samp.shape[0]), f32)
    for c in range(CHUNKS):
        copies[1 + c].wait()
        cols = slice(c * width, (c + 1) * width)
        w16 = jnp.broadcast_to(wrow[:, cols].astype(bf16), (16, width))
        acc = acc + dot_t(w16, samp[:, cols])
    rows = [acc[0:1, 128 * i : 128 * i + 128] for i in range(4)]
    mine = jnp.concatenate(rows + [jnp.zeros((4, 128), f32)], axis=0)
    part[...] = jnp.broadcast_to(mine[None], part.shape)
    copies[1 + CHUNKS].wait()
    copies[2 + CHUNKS].wait()

    @pl.when(lax.axis_index("core") == 1)
    def _():
        part[:, 4:8, :] = jnp.broadcast_to(gram_of(hist)[None], (part.shape[0], 4, 128))


def second_kernel(parts, labels, samp, hist, wrow, packed):
    summed = jnp.sum(parts[...], axis=0)
    feats = samp.shape[1]
    for i in range(4):
        packed[:, feats + 128 * i : feats + 128 * i + 128] = summed[4 + i : 5 + i]
    margin = jnp.concatenate([summed[i : i + 1] for i in range(4)], axis=1)
    resid = (jax.nn.sigmoid(margin) - labels[...].astype(f32)).astype(bf16)
    resid16 = jnp.broadcast_to(resid, (16, resid.shape[1]))
    width = 1024
    acc = jnp.zeros((2 * HIST, 128), f32)
    for c in range(feats // width):
        cols = slice(c * width, (c + 1) * width)
        t = jnp.dot(resid16, samp[:, cols], preferred_element_type=f32)[0:1]
        packed[:, cols] = t
        lead = wrow[:, cols] * 0.125 + penalty * t
        prod = hist[:, cols] * lead
        for k in range(width // 128):
            acc = acc + prod[:, 128 * k : 128 * k + 128]
    sums = jnp.sum(acc, axis=1, keepdims=True)
    here = iota(acc.shape, 0) == iota(acc.shape, 1)
    packed[:, feats + 512 :] = jnp.sum(jnp.where(here, sums, 0.0), axis=0, keepdims=True)


def spread_kernel(mine, other, cross_hbm, total, gram, cross, sem):
    feats = total.shape[1]
    line = mine[:, feats + 512 :] + other[:, feats + 512 :]
    cross[...] = jnp.broadcast_to(line[None], cross.shape)
    out = pltpu.make_async_copy(cross, cross_hbm, sem)
    out.start()
    total[...] = mine[:, :feats] + other[:, :feats]
    gram[...] = mine[:, feats : feats + 512] + other[:, feats : feats + 512]
    out.wait()


def solve_kernel(counter, gram, out):
    newest = lax.rem(counter[0], HIST)
    row = iota((HIST, 128), 0)
    lane = iota((HIST, 128), 1)
    low_lane = lane < HIST

    def unpacked(a):
        kept = jnp.where(iota((8, 128), 1) // HIST == iota((8, 128), 0), gram[:, 128 * a : 128 * a + 128], 0.0)
        for shift in (16, 32, 64):
            kept = kept + pltpu.roll(kept, shift, 1)
        return kept

    sy = jnp.where(low_lane, jnp.concatenate([unpacked(0), unpacked(1)], axis=0), 0.0)
    yy = jnp.where(low_lane, jnp.concatenate([unpacked(2), unpacked(3)], axis=0), 0.0)
    diag = row == lane
    is_new = jnp.logical_and(diag, row == newest)
    pick = lambda m: jnp.sum(jnp.sum(jnp.where(is_new, m, 0.0), axis=0, keepdims=True), axis=1, keepdims=True)
    gamma = pick(sy) / pick(yy)
    rank = lax.rem(newest - row + HIST, HIST)
    curv = jnp.sum(jnp.where(diag, sy, 0.0), axis=1, keepdims=True)
    rho = 1.0 / curv
    inv = diag.astype(f32)
    for step in range(HIST):
        here = row == lax.rem(newest - step + HIST, HIST)
        there = lane == lax.rem(newest - step + HIST, HIST)
        line = jnp.sum(jnp.where(here, inv * rho, 0.0), axis=0, keepdims=True)
        column = jnp.sum(jnp.where(there, sy, 0.0), axis=1, keepdims=True)
        later = inv - column * line
        inv = jnp.where(here, jnp.broadcast_to(line, inv.shape), jnp.where(rank > step, later, inv))
    pad = jnp.zeros((128 - HIST, 128), f32)
    inv_t = jnp.concatenate([inv, pad], axis=0).T[:HIST]
    middle = gamma * yy + jnp.where(diag, sy, 0.0)
    inner = jnp.dot(middle, jnp.concatenate([inv, pad], axis=0), precision=highest, preferred_element_type=f32)
    corner = jnp.dot(inv_t, jnp.concatenate([inner, pad], axis=0), precision=highest, preferred_element_type=f32)
    out[0:HIST, :] = corner - gamma * pltpu.roll(inv_t, HIST, 1)
    out[HIST : 2 * HIST, :] = -gamma * inv
    out[2 * HIST :, :] = jnp.broadcast_to(gamma, (8, 128))


def last_kernel(crosses, solve, mine, other, wrow, hist, new_weights, gradient):
    line = jnp.sum(jnp.sum(crosses[...], axis=0), axis=0, keepdims=True)
    coefs = step_length * jnp.sum(solve[0 : 2 * HIST, :] * line, axis=1, keepdims=True)
    weights = wrow[...]
    grad = weights + penalty * (mine[...] + other[...])
    gradient[...] = grad
    base = weights - (step_length * solve[2 * HIST : 2 * HIST + 1, 0:1]) * grad
    new_weights[...] = base - jnp.sum(hist[...] * coefs, axis=0, keepdims=True)


def swapped(array, mask):
    count = lax.axis_size(ROWS)
    return lax.ppermute(array, ROWS, [(i, i ^ mask) for i in range(count)])


SMALL = pltpu.CompilerParams(vmem_limit_bytes=16 * 1024 * 1024)
VM = pl.BlockSpec(memory_space=pltpu.VMEM)
HB = pl.BlockSpec(memory_space=pltpu.HBM)


def body(samples, labels, weights, hist_s, hist_y, counter):
    count, feats = samples.shape
    samp, hist, wrow, part = pl.pallas_call(
        first_kernel,
        in_specs=[HB] * 4,
        out_specs=[VM] * 4,
        out_shape=[
            pltpu.VMEM((count, feats), bf16),
            pltpu.VMEM((2 * HIST, feats), f32),
            pltpu.VMEM((1, feats), f32),
            pltpu.VMEM((16, 8, 128), f32),
        ],
        scratch_shapes=[pltpu.SemaphoreType.DMA((3 + CHUNKS,))],
        compiler_params=SMALL,
        name="first",
    )(*(pltpu.with_memory_space_constraint(a, pltpu.HBM) for a in (samples, weights.reshape(1, feats), hist_s, hist_y)))
    parts = lax.all_to_all(part, COLS, split_axis=0, concat_axis=0, axis_index_groups=[list(range(15, -1, -1))], tiled=True)
    packed = pl.pallas_call(
        second_kernel,
        in_specs=[VM] * 5,
        out_specs=VM,
        out_shape=pltpu.VMEM((1, feats + 640), f32),
        compiler_params=SMALL,
        name="second",
    )(parts, labels.reshape(1, count), samp, hist, wrow)
    other = swapped(packed, 1)
    cross, total, gram = pl.pallas_call(
        spread_kernel,
        in_specs=[VM] * 2,
        out_specs=[HB, VM, VM],
        out_shape=[
            jax.ShapeDtypeStruct((8, 8, 128), f32),
            pltpu.VMEM((1, feats), f32),
            pltpu.VMEM((1, 512), f32),
        ],
        scratch_shapes=[pltpu.VMEM((8, 8, 128), f32), pltpu.SemaphoreType.DMA],
        compiler_params=SMALL,
        name="spread",
    )(packed, other)
    crosses = lax.all_to_all(cross.reshape(64, 1, 128), ("x", COLS), split_axis=0, concat_axis=0, axis_index_groups=[[63] + list(range(63))], tiled=True)
    other = swapped(total, 3)
    total = total + other
    other = swapped(total, 6)
    solve = pl.pallas_call(
        solve_kernel,
        in_specs=[pl.BlockSpec(memory_space=pltpu.SMEM), VM],
        out_specs=VM,
        out_shape=pltpu.VMEM((40, 128), f32),
        compiler_params=SMALL,
        name="solve",
    )(counter, gram)
    new_weights, gradient = pl.pallas_call(
        last_kernel,
        in_specs=[VM] * 6,
        out_specs=[VM] * 2,
        out_shape=[jax.ShapeDtypeStruct((1, feats), f32)] * 2,
        compiler_params=SMALL,
        name="last",
    )(crosses.reshape(8, 8, 128), solve, total, other, wrow, hist)
    return new_weights.reshape(feats), gradient.reshape(feats)


def solution(mesh):
    split = Mesh(mesh.devices.reshape(4, 2, 16), ("x", "core", COLS))
    return jax.shard_map(
        body,
        mesh=split,
        in_specs=(P(ROWS, COLS), P(ROWS), P(COLS), P(None, COLS), P(None, COLS), P()),
        out_specs=(P(COLS), P(COLS)),
        check_vma=False,
    )
```

```python
import jax
import jax.numpy as jnp
from jax import lax
from jax.experimental import pallas as pl
from jax.experimental.pallas import tpu as pltpu
from jax.sharding import Mesh
from jax.sharding import PartitionSpec as P


HIST = 16
ROWS = ("x", "core")
COLS = "cols"
CHUNKS = 16

penalty = 4.0
step_length = 0.5
f32 = jnp.float32
bf16 = jnp.bfloat16
highest = lax.Precision.HIGHEST


def iota(shape, axis):
    return lax.broadcasted_iota(jnp.int32, shape, axis)


def dot_t(left, right):
    return lax.dot_general(left, right, (((1,), (1,)), ((), ())), preferred_element_type=f32)


def gram_of(hist):
    h = hist[...]
    high = h.astype(bf16)
    low = (h - high.astype(f32)).astype(bf16)
    both = dot_t(jnp.concatenate([high, low], axis=0), jnp.concatenate([high[HIST:], low[HIST:]], axis=0))
    both = jnp.concatenate([both, jnp.zeros((4 * HIST, 128 - 2 * HIST), f32)], axis=1)
    halves = both[: 2 * HIST] + both[2 * HIST :]
    lane = iota((2 * HIST, 128), 1)
    gram = jnp.where(lane < HIST, halves + pltpu.roll(halves, 128 - HIST, 1), 0.0)
    for shift in (16, 32, 64):
        gram = gram + pltpu.roll(gram, shift, 1)
    gram = jnp.where(lane // HIST == iota((2 * HIST, 128), 0) % 8, gram, 0.0)
    return jnp.concatenate([jnp.sum(gram[8 * a : 8 * a + 8], axis=0, keepdims=True) for a in range(4)], axis=0)


def first_kernel(s_hbm, w_hbm, hs_hbm, hy_hbm, samp, hist, wrow, part, sems):
    feats = samp.shape[1]
    width = feats // CHUNKS
    copies = [pltpu.make_async_copy(w_hbm, wrow, sems.at[0])]
    for c in range(CHUNKS):
        cols = pl.ds(c * width, width)
        copies.append(pltpu.make_async_copy(s_hbm.at[:, cols], samp.at[:, cols], sems.at[1 + c]))
    copies.append(pltpu.make_async_copy(hs_hbm, hist.at[pl.ds(0, HIST), :], sems.at[1 + CHUNKS]))
    copies.append(pltpu.make_async_copy(hy_hbm, hist.at[pl.ds(HIST, HIST), :], sems.at[2 + CHUNKS]))
    for copy in copies:
        copy.start()
    copies[0].wait()
    acc = jnp.zeros((16, samp.shape[0]), f32)
    for c in range(CHUNKS):
        copies[1 + c].wait()
        cols = slice(c * width, (c + 1) * width)
        w16 = jnp.broadcast_to(wrow[:, cols].astype(bf16), (16, width))
        acc = acc + dot_t(w16, samp[:, cols])
    rows = [acc[0:1, 128 * i : 128 * i + 128] for i in range(4)]
    mine = jnp.concatenate(rows + [jnp.zeros((4, 128), f32)], axis=0)
    part[...] = jnp.broadcast_to(mine[None], part.shape)
    copies[1 + CHUNKS].wait()
    copies[2 + CHUNKS].wait()

    @pl.when(lax.axis_index("core") == 1)
    def _():
        part[:, 4:8, :] = jnp.broadcast_to(gram_of(hist)[None], (part.shape[0], 4, 128))


def second_kernel(parts, labels, samp, hist, wrow, packed):
    summed = jnp.sum(parts[...], axis=0)
    feats = samp.shape[1]
    for i in range(4):
        packed[:, feats + 128 * i : feats + 128 * i + 128] = summed[4 + i : 5 + i]
    margin = jnp.concatenate([summed[i : i + 1] for i in range(4)], axis=1)
    resid = (jax.nn.sigmoid(margin) - labels[...].astype(f32)).astype(bf16)
    resid16 = jnp.broadcast_to(resid, (16, resid.shape[1]))
    width = 1024
    acc = jnp.zeros((2 * HIST, 128), f32)
    for c in range(feats // width):
        cols = slice(c * width, (c + 1) * width)
        t = jnp.dot(resid16, samp[:, cols], preferred_element_type=f32)[0:1]
        packed[:, cols] = t
        lead = wrow[:, cols] * 0.125 + penalty * t
        prod = hist[:, cols] * lead
        for k in range(width // 128):
            acc = acc + prod[:, 128 * k : 128 * k + 128]
    sums = jnp.sum(acc, axis=1, keepdims=True)
    here = iota(acc.shape, 0) == iota(acc.shape, 1)
    packed[:, feats + 512 :] = jnp.sum(jnp.where(here, sums, 0.0), axis=0, keepdims=True)


def spread_kernel(mine, other, cross_hbm, total, gram, cross, sem):
    feats = total.shape[1]
    line = mine[:, feats + 512 :] + other[:, feats + 512 :]
    cross[...] = jnp.broadcast_to(line[None], cross.shape)
    out = pltpu.make_async_copy(cross, cross_hbm, sem)
    out.start()
    total[...] = mine[:, :feats] + other[:, :feats]
    gram[...] = mine[:, feats : feats + 512] + other[:, feats : feats + 512]
    out.wait()


def solve_kernel(counter, gram, out):
    newest = lax.rem(counter[0], HIST)
    row = iota((HIST, 128), 0)
    lane = iota((HIST, 128), 1)
    low_lane = lane < HIST

    def unpacked(a):
        kept = jnp.where(iota((8, 128), 1) // HIST == iota((8, 128), 0), gram[:, 128 * a : 128 * a + 128], 0.0)
        for shift in (16, 32, 64):
            kept = kept + pltpu.roll(kept, shift, 1)
        return kept

    sy = jnp.where(low_lane, jnp.concatenate([unpacked(0), unpacked(1)], axis=0), 0.0)
    yy = jnp.where(low_lane, jnp.concatenate([unpacked(2), unpacked(3)], axis=0), 0.0)
    diag = row == lane
    is_new = jnp.logical_and(diag, row == newest)
    pick = lambda m: jnp.sum(jnp.sum(jnp.where(is_new, m, 0.0), axis=0, keepdims=True), axis=1, keepdims=True)
    gamma = pick(sy) / pick(yy)
    rank = lax.rem(newest - row + HIST, HIST)
    curv = jnp.sum(jnp.where(diag, sy, 0.0), axis=1, keepdims=True)
    rho = 1.0 / curv
    inv = diag.astype(f32)
    for step in range(HIST):
        here = row == lax.rem(newest - step + HIST, HIST)
        there = lane == lax.rem(newest - step + HIST, HIST)
        line = jnp.sum(jnp.where(here, inv * rho, 0.0), axis=0, keepdims=True)
        column = jnp.sum(jnp.where(there, sy, 0.0), axis=1, keepdims=True)
        later = inv - column * line
        inv = jnp.where(here, jnp.broadcast_to(line, inv.shape), jnp.where(rank > step, later, inv))
    pad = jnp.zeros((128 - HIST, 128), f32)
    inv_t = jnp.concatenate([inv, pad], axis=0).T[:HIST]
    middle = gamma * yy + jnp.where(diag, sy, 0.0)
    inner = jnp.dot(middle, jnp.concatenate([inv, pad], axis=0), precision=highest, preferred_element_type=f32)
    corner = jnp.dot(inv_t, jnp.concatenate([inner, pad], axis=0), precision=highest, preferred_element_type=f32)
    out[0:HIST, :] = corner - gamma * pltpu.roll(inv_t, HIST, 1)
    out[HIST : 2 * HIST, :] = -gamma * inv
    out[2 * HIST :, :] = jnp.broadcast_to(gamma, (8, 128))


def last_kernel(crosses, solve, mine, other, wrow, hist, new_hbm, grad_hbm, new, gradient, sems):
    feats = wrow.shape[1]
    weights = wrow[...]
    grad = weights + penalty * (mine[...] + other[...])
    gradient[...] = grad
    outs = [pltpu.make_async_copy(gradient, grad_hbm, sems.at[0])]
    outs[0].start()
    line = jnp.sum(jnp.sum(crosses[...], axis=0), axis=0, keepdims=True)
    coefs = step_length * jnp.sum(solve[0 : 2 * HIST, :] * line, axis=1, keepdims=True)
    gamma = step_length * solve[2 * HIST : 2 * HIST + 1, 0:1]
    for i in range(2):
        cols = slice(i * feats // 2, (i + 1) * feats // 2)
        mixed = jnp.sum(hist[:, cols] * coefs, axis=0, keepdims=True)
        new[:, cols] = wrow[:, cols] - gamma * grad[:, cols] - mixed
        half = pl.ds(i * feats // 2, feats // 2)
        outs.append(pltpu.make_async_copy(new.at[:, half], new_hbm.at[:, half], sems.at[1 + i]))
        outs[-1].start()
    for out in outs:
        out.wait()


def swapped(array, mask):
    count = lax.axis_size(ROWS)
    return lax.ppermute(array, ROWS, [(i, i ^ mask) for i in range(count)])


SMALL = pltpu.CompilerParams(vmem_limit_bytes=16 * 1024 * 1024)
VM = pl.BlockSpec(memory_space=pltpu.VMEM)
HB = pl.BlockSpec(memory_space=pltpu.HBM)


def body(samples, labels, weights, hist_s, hist_y, counter):
    count, feats = samples.shape
    samp, hist, wrow, part = pl.pallas_call(
        first_kernel,
        in_specs=[HB] * 4,
        out_specs=[VM] * 4,
        out_shape=[
            pltpu.VMEM((count, feats), bf16),
            pltpu.VMEM((2 * HIST, feats), f32),
            pltpu.VMEM((1, feats), f32),
            pltpu.VMEM((16, 8, 128), f32),
        ],
        scratch_shapes=[pltpu.SemaphoreType.DMA((3 + CHUNKS,))],
        compiler_params=SMALL,
        name="first",
    )(*(pltpu.with_memory_space_constraint(a, pltpu.HBM) for a in (samples, weights.reshape(1, feats), hist_s, hist_y)))
    parts = lax.all_to_all(part, COLS, split_axis=0, concat_axis=0, axis_index_groups=[list(range(15, -1, -1))], tiled=True)
    packed = pl.pallas_call(
        second_kernel,
        in_specs=[VM] * 5,
        out_specs=VM,
        out_shape=pltpu.VMEM((1, feats + 640), f32),
        compiler_params=SMALL,
        name="second",
    )(parts, labels.reshape(1, count), samp, hist, wrow)
    other = swapped(packed, 1)
    cross, total, gram = pl.pallas_call(
        spread_kernel,
        in_specs=[VM] * 2,
        out_specs=[HB, VM, VM],
        out_shape=[
            jax.ShapeDtypeStruct((8, 8, 128), f32),
            pltpu.VMEM((1, feats), f32),
            pltpu.VMEM((1, 512), f32),
        ],
        scratch_shapes=[pltpu.VMEM((8, 8, 128), f32), pltpu.SemaphoreType.DMA],
        compiler_params=SMALL,
        name="spread",
    )(packed, other)
    crosses = lax.all_to_all(cross.reshape(64, 1, 128), ("x", COLS), split_axis=0, concat_axis=0, axis_index_groups=[[63] + list(range(63))], tiled=True)
    other = swapped(total, 3)
    total = total + other
    other = swapped(total, 6)
    solve = pl.pallas_call(
        solve_kernel,
        in_specs=[pl.BlockSpec(memory_space=pltpu.SMEM), VM],
        out_specs=VM,
        out_shape=pltpu.VMEM((40, 128), f32),
        compiler_params=SMALL,
        name="solve",
    )(counter, gram)
    new_weights, gradient = pl.pallas_call(
        last_kernel,
        in_specs=[VM] * 6,
        out_specs=[HB] * 2,
        out_shape=[jax.ShapeDtypeStruct((1, feats), f32)] * 2,
        scratch_shapes=[pltpu.VMEM((1, feats), f32), pltpu.VMEM((1, feats), f32), pltpu.SemaphoreType.DMA((3,))],
        compiler_params=SMALL,
        name="last",
    )(crosses.reshape(8, 8, 128), solve, total, other, wrow, hist)
    return new_weights.reshape(feats), gradient.reshape(feats)


def solution(mesh):
    split = Mesh(mesh.devices.reshape(4, 2, 16), ("x", "core", COLS))
    return jax.shard_map(
        body,
        mesh=split,
        in_specs=(P(ROWS, COLS), P(ROWS), P(COLS), P(None, COLS), P(None, COLS), P()),
        out_specs=(P(COLS), P(COLS)),
        check_vma=False,
    )
```
